128 devices in a mesh: row: 8 (over y, z_lo), col: 16 (over z_hi, x, core).
Axes of the slice: x: 4, y: 4, z: 4 (z_hi: 2, z_lo: 2; z = z_hi * 2 + z_lo), core: 2. Of those that a mesh axis runs over, the one named last changes fastest.
Arguments:
- homolog_stack: bfloat16 [512, 512, 256], P(('row', 'col')), may hold values from -6 to 6
- per_amino_features: bfloat16 [512, 256], P(('row', 'col')), may hold values from -6 to 6
- asking_matrix: bfloat16 [256, 256], replicated, may hold values from -24 to 24
- lookup_matrix: bfloat16 [256, 256], replicated, may hold values from -0.375 to 0.375
- content_matrix: bfloat16 [256, 256], replicated, may hold values from -0.375 to 0.375
- sigmoid_scaling_matrix: bfloat16 [256, 256], replicated, may hold values from -0.375 to 0.375
- attention_result_matrix: bfloat16 [256, 256], replicated, may hold values from -0.375 to 0.375
- stack_transition_expand_matrix: bfloat16 [256, 1024], replicated, may hold values from -0.375 to 0.375
- stack_transition_shrink_matrix: bfloat16 [1024, 256], replicated, may hold values from -0.1875 to 0.1875
- former_factor_matrix: bfloat16 [256, 32], replicated, may hold values from -0.375 to 0.375
- latter_factor_matrix: bfloat16 [256, 32], replicated, may hold values from -0.375 to 0.375
- factor_mean_projection: bfloat16 [1024, 128], replicated, may hold values from -1.1953125 to 1.1953125
- row_amino_embedding: bfloat16 [256, 128], replicated, may hold values from -0.375 to 0.375
- column_amino_embedding: bfloat16 [256, 128], replicated, may hold values from -0.375 to 0.375
- offset_embedding_matrix: bfloat16 [65, 128], replicated, may hold values from -3 to 3
- grid_transition_expand: bfloat16 [128, 512], replicated, may hold values from -0.5 to 0.5
- grid_transition_shrink: bfloat16 [512, 128], replicated, may hold values from -0.25 to 0.25
- distance_bins_matrix: bfloat16 [128, 64], replicated, may hold values from -0.5 to 0.5
Outputs:
- alignment_output: bfloat16 [512, 512, 256], P(None, ('row', 'col'))
- pair_output: bfloat16 [512, 512, 128], P('row', 'col')
- distogram: bfloat16 [512, 512, 64], P('row', 'col')
The draws below stay inside these ranges and needn't reach their ends.
All inputs are finite; a program needn't handle non-finite values.
Results may differ from the reference program's by a relative error of at most 0.011.
The reference program's roundings to bfloat16 on the way count: a program that leaves them out, or rounds other values in their place, can miss the bound.
Values may be sent and summed in bfloat16 or wider, within the bound.
A program may use at most 256 MiB of HBM per device.

```python
import math
import jax
import jax.numpy as jnp
from jax import lax

STACK_FEATURES = 256
HEADS = 8
HEAD = 32
STACK_INNER = 1024
FACTOR_WIDTH = 32
GRID_FEATURES = 128
PAIR_HIDDEN = 512
BINS = 64
CLIP = 32
HOMOLOG_TOTAL = 512
AMINO_TOTAL = 512


def draw_asking_matrix(key, part):
    starting_tensor = jnp.clip(jax.random.normal(key, (STACK_FEATURES, STACK_FEATURES), jnp.float32), -4.0, 4.0)
    result = starting_tensor * 0.0625
    return result.astype(jnp.bfloat16)


def steps_of(rng, shape, cuts, least, high):
    def one(position, parts):
        steps = jax.random.uniform(jax.random.fold_in(jax.random.fold_in(rng, 6), position), (parts,), jnp.float32, least / len(cuts), high / len(cuts))
        return jnp.repeat(jnp.exp(steps), shape[position] // parts).reshape((-1,) + (1,) * (len(shape) - position - 1))

    loudness = one(*cuts[0])
    for cut in cuts[1:]:
        loudness = loudness * one(*cut)
    return loudness


def gaussian(stream_key, shape, scale, reach, shards=(), held_as=jnp.bfloat16):
    array = jax.random.normal(stream_key, shape, jnp.float32) * scale
    if len(shards) > 0:
        array = steps_of(stream_key, shape, shards, -0.22, 0.18) * array
    return jnp.clip(array, min=-reach, max=reach).astype(held_as)


def setup_inputs(seed: int = 0) -> dict:
    streams_of = jax.random.split(jax.random.key(seed), 19)
    homolog_stack = gaussian(streams_of[0], (HOMOLOG_TOTAL, AMINO_TOTAL, STACK_FEATURES), 1.0, 6.0, ((0, 128),))
    per_amino_features = gaussian(streams_of[1], (AMINO_TOTAL, STACK_FEATURES), 1.0, 6.0, ((0, 128),))
    asking_matrix = draw_asking_matrix(jax.random.fold_in(streams_of[18], 71), 0)
    lookup_matrix = gaussian(streams_of[3], (STACK_FEATURES, STACK_FEATURES), STACK_FEATURES ** -0.5, 0.375)
    content_matrix = gaussian(streams_of[4], (STACK_FEATURES, STACK_FEATURES), STACK_FEATURES ** -0.5, 0.375)
    sigmoid_scaling_matrix = gaussian(streams_of[5], (STACK_FEATURES, STACK_FEATURES), STACK_FEATURES ** -0.5, 0.375)
    attention_result_matrix = gaussian(streams_of[6], (STACK_FEATURES, STACK_FEATURES), STACK_FEATURES ** -0.5, 0.375)
    stack_transition_expand_matrix = gaussian(streams_of[7], (STACK_FEATURES, STACK_INNER), STACK_FEATURES ** -0.5, 0.375)
    stack_transition_shrink_matrix = gaussian(streams_of[8], (STACK_INNER, STACK_FEATURES), STACK_INNER ** -0.5, 0.1875)
    former_factor_matrix = gaussian(streams_of[9], (STACK_FEATURES, FACTOR_WIDTH), STACK_FEATURES ** -0.5, 0.375)
    latter_factor_matrix = gaussian(streams_of[10], (STACK_FEATURES, FACTOR_WIDTH), STACK_FEATURES ** -0.5, 0.375)
    factor_mean_projection = gaussian(streams_of[11], (FACTOR_WIDTH * FACTOR_WIDTH, GRID_FEATURES), 0.2, 1.1953125)
    row_amino_embedding = gaussian(streams_of[12], (STACK_FEATURES, GRID_FEATURES), STACK_FEATURES ** -0.5, 0.375)
    column_amino_embedding = gaussian(streams_of[13], (STACK_FEATURES, GRID_FEATURES), STACK_FEATURES ** -0.5, 0.375)
    offset_embedding_matrix = gaussian(streams_of[14], (2 * CLIP + 1, GRID_FEATURES), 0.5, 3.0)
    grid_transition_expand = gaussian(streams_of[15], (GRID_FEATURES, PAIR_HIDDEN), GRID_FEATURES ** -0.5, 0.5)
    grid_transition_shrink = gaussian(streams_of[16], (PAIR_HIDDEN, GRID_FEATURES), PAIR_HIDDEN ** -0.5, 0.25)
    distance_bins_matrix = gaussian(streams_of[17], (GRID_FEATURES, BINS), GRID_FEATURES ** -0.5, 0.5)
    return {"homolog_stack": homolog_stack, "per_amino_features": per_amino_features, "asking_matrix": asking_matrix, "lookup_matrix": lookup_matrix, "content_matrix": content_matrix, "sigmoid_scaling_matrix": sigmoid_scaling_matrix, "attention_result_matrix": attention_result_matrix, "stack_transition_expand_matrix": stack_transition_expand_matrix, "stack_transition_shrink_matrix": stack_transition_shrink_matrix, "former_factor_matrix": former_factor_matrix, "latter_factor_matrix": latter_factor_matrix, "factor_mean_projection": factor_mean_projection, "row_amino_embedding": row_amino_embedding, "column_amino_embedding": column_amino_embedding, "offset_embedding_matrix": offset_embedding_matrix, "grid_transition_expand": grid_transition_expand, "grid_transition_shrink": grid_transition_shrink, "distance_bins_matrix": distance_bins_matrix}


def standardize_features(values):
    middle = lax.optimization_barrier(jnp.mean(values, -1, keepdims=True))
    centred = values - middle
    spread = lax.optimization_barrier(jnp.mean(centred * centred, -1, keepdims=True))
    return centred * lax.rsqrt(spread + 1e-05)

def alignment_layer(block_piece, asking_matrix, lookup_matrix, content_matrix, sigmoid_scaling_matrix, attention_result_matrix, stack_transition_expand_matrix, stack_transition_shrink_matrix):
    count_seq, count_res, feature_width = block_piece.shape
    start = block_piece.astype(jnp.float32).reshape(-1, feature_width)
    standardized = standardize_features(start).astype(jnp.bfloat16)
    query = jnp.dot(standardized, asking_matrix, preferred_element_type=jnp.float32).astype(jnp.bfloat16)
    key_rows = jnp.dot(standardized, lookup_matrix, preferred_element_type=jnp.float32).astype(jnp.bfloat16)
    value_rows = jnp.dot(standardized, content_matrix, preferred_element_type=jnp.float32).astype(jnp.bfloat16)
    gate = jax.nn.sigmoid(jnp.dot(standardized, sigmoid_scaling_matrix, preferred_element_type=jnp.float32))
    query = query.reshape(count_seq, count_res, HEADS, HEAD).astype(jnp.float32)
    key_rows = key_rows.reshape(count_seq, count_res, HEADS, HEAD).astype(jnp.float32)
    value_rows = value_rows.reshape(count_seq, count_res, HEADS, HEAD).astype(jnp.float32)
    scores = jnp.einsum('sihd,tihd->ihst', query, key_rows) / math.sqrt(HEAD)
    weights = jax.nn.softmax(scores, -1).astype(jnp.bfloat16).astype(jnp.float32)
    attended = jnp.einsum('ihst,tihd->sihd', weights, value_rows).reshape(-1, feature_width)
    mixed = (attended * gate).astype(jnp.bfloat16)
    first_part = start + jnp.dot(mixed, attention_result_matrix, preferred_element_type=jnp.float32)
    hidden_units = jax.nn.relu(jnp.dot(standardize_features(first_part).astype(jnp.bfloat16), stack_transition_expand_matrix, preferred_element_type=jnp.float32)).astype(jnp.bfloat16)
    second_part = first_part + jnp.dot(hidden_units, stack_transition_shrink_matrix, preferred_element_type=jnp.float32)
    return second_part.reshape(count_seq, count_res, feature_width)

def pair_block(a_u, b_v, left_u, right_v, start_u, start_v, offset_embedding_matrix, factor_mean_projection, grid_transition_expand, grid_transition_shrink, distance_bins_matrix):
    count_seq, count_u, factor = a_u.shape
    count_v = b_v.shape[1]
    feature_width = left_u.shape[1]
    step_rows = max(1, min(count_u, 1024 // count_v))
    tile_collection = count_u // step_rows
    a_blocks = a_u.reshape(count_seq, tile_collection, step_rows, factor).transpose(1, 0, 2, 3)
    left_blocks = left_u.reshape(tile_collection, step_rows, feature_width)
    flat_v = b_v.reshape(count_seq, count_v * factor)
    columns = start_v + jnp.arange(count_v, dtype=jnp.int32)
    bins = jnp.arange(2 * CLIP + 1, dtype=jnp.int32)

    def one_block(inputs):
        a_blk, left_blk, index = inputs
        outer = lax.dot_general(a_blk.reshape(count_seq, step_rows * factor), flat_v, (((0,), (0,)), ((), ())), preferred_element_type=jnp.float32)
        outer = outer.reshape(step_rows, factor, count_v, factor).transpose(0, 2, 1, 3).reshape(step_rows * count_v, factor * factor)
        outer = (outer / count_seq).astype(jnp.bfloat16)
        projected = jnp.dot(outer, factor_mean_projection, preferred_element_type=jnp.float32)
        rows_here = start_u + index * step_rows + jnp.arange(step_rows, dtype=jnp.int32)
        offset = jnp.clip(columns[None, :] - rows_here[:, None], -CLIP, CLIP) + CLIP
        onehot = (offset[:, :, None] == bins).astype(jnp.bfloat16).reshape(-1, 2 * CLIP + 1)
        relative = jnp.dot(onehot, offset_embedding_matrix, preferred_element_type=jnp.float32)
        embedded = (left_blk.astype(jnp.float32)[:, None, :] + right_v.astype(jnp.float32)[None, :, :]).reshape(-1, feature_width)
        start_pair = embedded + relative + projected
        hidden_units = jax.nn.relu(jnp.dot(standardize_features(start_pair).astype(jnp.bfloat16), grid_transition_expand, preferred_element_type=jnp.float32)).astype(jnp.bfloat16)
        final = start_pair + jnp.dot(hidden_units, grid_transition_shrink, preferred_element_type=jnp.float32)
        rounded = final.astype(jnp.bfloat16)
        logits = jnp.dot(rounded, distance_bins_matrix, preferred_element_type=jnp.float32)
        return (rounded.reshape(step_rows, count_v, feature_width), logits.reshape(step_rows, count_v, -1))
    pairs, logits = lax.map(one_block, (a_blocks, left_blocks, jnp.arange(tile_collection, dtype=jnp.int32)))
    return (pairs.reshape(count_u, count_v, feature_width), logits.reshape(count_u, count_v, -1))

def reference(homolog_stack, per_amino_features, asking_matrix, lookup_matrix, content_matrix, sigmoid_scaling_matrix, attention_result_matrix, stack_transition_expand_matrix, stack_transition_shrink_matrix, former_factor_matrix, latter_factor_matrix, factor_mean_projection, row_amino_embedding, column_amino_embedding, offset_embedding_matrix, grid_transition_expand, grid_transition_shrink, distance_bins_matrix):
    tile_collection = 16
    divide_into_fragments = homolog_stack.reshape(HOMOLOG_TOTAL, tile_collection, AMINO_TOTAL // tile_collection, STACK_FEATURES).transpose(1, 0, 2, 3)
    refreshed_stack = lax.map(lambda partial_block: alignment_layer(partial_block, asking_matrix, lookup_matrix, content_matrix, sigmoid_scaling_matrix, attention_result_matrix, stack_transition_expand_matrix, stack_transition_shrink_matrix), divide_into_fragments)
    refreshed_stack = refreshed_stack.transpose(1, 0, 2, 3).reshape(HOMOLOG_TOTAL, AMINO_TOTAL, STACK_FEATURES)
    alignment_output = refreshed_stack.astype(jnp.bfloat16)
    standardized = standardize_features(refreshed_stack).astype(jnp.bfloat16).reshape(-1, STACK_FEATURES)
    left_opm = jnp.dot(standardized, former_factor_matrix, preferred_element_type=jnp.float32).astype(jnp.bfloat16).reshape(HOMOLOG_TOTAL, AMINO_TOTAL, FACTOR_WIDTH)
    right_opm = jnp.dot(standardized, latter_factor_matrix, preferred_element_type=jnp.float32).astype(jnp.bfloat16).reshape(HOMOLOG_TOTAL, AMINO_TOTAL, FACTOR_WIDTH)
    left_pair = jnp.dot(per_amino_features, row_amino_embedding, preferred_element_type=jnp.float32).astype(jnp.bfloat16)
    right_pair = jnp.dot(per_amino_features, column_amino_embedding, preferred_element_type=jnp.float32).astype(jnp.bfloat16)
    pair_output, logits = pair_block(left_opm, right_opm, left_pair, right_pair, 0, 0, offset_embedding_matrix, factor_mean_projection, grid_transition_expand, grid_transition_shrink, distance_bins_matrix)
    distogram = (logits + logits.transpose(1, 0, 2)).astype(jnp.bfloat16)
    return (alignment_output, pair_output, distogram)
```

```python
import functools
import math

import jax
import jax.numpy as jnp
from jax import lax
from jax.experimental import pallas as pl
from jax.experimental.pallas import tpu as pltpu
from jax.sharding import PartitionSpec as P

HEADS = 8
HEAD = 32
CLIP = 32
MESH = pl.DeviceIdType.MESH
FULL = pl.BlockSpec(memory_space=pltpu.VMEM)


def standardize_features(values):
    middle = jnp.mean(values, -1, keepdims=True)
    centred = values - middle
    spread = jnp.mean(centred * centred, -1, keepdims=True)
    return centred * lax.rsqrt(spread + 1e-05)


def mm(a, b):
    return jnp.dot(a, b, preferred_element_type=jnp.float32)


def column_attention(
    x_ref,
    feat_ref,
    wq_ref,
    wk_ref,
    wv_ref,
    wg_ref,
    wo_ref,
    we_ref,
    ws_ref,
    factor_ref,
    row_ref,
    column_ref,
    out_ref,
    a_ref,
    b_ref,
    q_scr,
    kt_scr,
    v_scr,
    acc_scr,
    fac_scr,
):
    step = pl.program_id(0)
    seqs = x_ref.shape[1]
    x = x_ref[0].astype(jnp.float32)
    normed = standardize_features(x).astype(jnp.bfloat16)
    q_scr[...] = mm(normed, wq_ref[...]).astype(jnp.bfloat16)
    kt_scr[...] = mm(normed, wk_ref[...]).T.astype(jnp.bfloat16)
    v = mm(normed, wv_ref[...]).astype(jnp.bfloat16)
    ones = jnp.ones((seqs, 128), jnp.bfloat16)
    v_scr[0] = jnp.concatenate([v[:, :128], ones], axis=1)
    v_scr[1] = jnp.concatenate([v[:, 128:], ones], axis=1)
    acc_scr[...] = jnp.zeros_like(acc_scr)
    lane = lax.broadcasted_iota(jnp.int32, (seqs, 256), 1)
    factor = math.log2(math.e) / math.sqrt(HEAD)

    def one_head(h, carry):
        group = h // 4
        q = jnp.where(lane // HEAD == h, q_scr[...], jnp.zeros((), jnp.bfloat16))
        scores = mm(q, kt_scr[...])
        top = jnp.max(scores, axis=-1, keepdims=True)
        weights = jnp.exp2((scores - top) * factor).astype(jnp.bfloat16)
        values = jnp.where(
            lane % 128 // HEAD == h % 4, v_scr[group], jnp.zeros((), jnp.bfloat16)
        )
        acc_scr[group] += mm(weights, values)
        return carry

    lax.fori_loop(0, HEADS, one_head, 0)
    attended = jnp.concatenate(
        [
            acc_scr[0, :, :128] / acc_scr[0, :, 128:],
            acc_scr[1, :, :128] / acc_scr[1, :, 128:],
        ],
        axis=1,
    )
    gate = jax.nn.sigmoid(mm(normed, wg_ref[...]))
    mixed = (attended * gate).astype(jnp.bfloat16)
    first = x + mm(mixed, wo_ref[...])
    hidden = jnp.maximum(
        mm(standardize_features(first).astype(jnp.bfloat16), we_ref[...]), 0.0
    ).astype(jnp.bfloat16)
    second = first + mm(hidden, ws_ref[...])
    out_ref[...] = second.astype(jnp.bfloat16)
    factors = mm(standardize_features(second).astype(jnp.bfloat16), factor_ref[...])
    fac_scr[...] = jnp.where(lane % 128 // HEAD == step, factors, fac_scr[...])

    @pl.when(step == pl.num_programs(0) - 1)
    def _():
        a_ref[:seqs, :] = fac_scr[:, :128].astype(jnp.bfloat16)
        b_ref[:128, :] = fac_scr[:, 128:].T.astype(jnp.bfloat16)
        feat = feat_ref[...]
        a_ref[seqs:, :] = mm(feat, row_ref[...]).astype(jnp.bfloat16)
        b_ref[128:, :128] = mm(feat, column_ref[...]).astype(jnp.bfloat16)
        b_ref[128:, 128:] = jnp.zeros((16, seqs - 128), jnp.bfloat16)


def run_attention(x, feat, weights, interpret=False):
    count_res, seqs, width = x.shape
    whole = [FULL] * (1 + len(weights))
    return pl.pallas_call(
        column_attention,
        grid=(count_res,),
        in_specs=[pl.BlockSpec((1, seqs, width), lambda i: (i, 0, 0))] + whole,
        out_specs=[
            pl.BlockSpec((seqs, width), lambda i: (0, i)),
            pl.BlockSpec((seqs + 16, 128), lambda i: (0, 0)),
            pl.BlockSpec((144, seqs), lambda i: (0, 0)),
        ],
        out_shape=[
            jax.ShapeDtypeStruct((seqs, count_res * width), jnp.bfloat16),
            jax.ShapeDtypeStruct((seqs + 16, 128), jnp.bfloat16),
            jax.ShapeDtypeStruct((144, seqs), jnp.bfloat16),
        ],
        scratch_shapes=[
            pltpu.VMEM((seqs, width), jnp.bfloat16),
            pltpu.VMEM((width, seqs), jnp.bfloat16),
            pltpu.VMEM((2, seqs, width), jnp.bfloat16),
            pltpu.VMEM((2, seqs, width), jnp.float32),
            pltpu.VMEM((seqs, width), jnp.float32),
        ],
        compiler_params=pltpu.CompilerParams(
            dimension_semantics=("arbitrary",), vmem_limit_bytes=48 * 1024 * 1024
        ),
        name="column_attention",
    )(x, feat, *weights)


def spread_factors(a_ref, b_ref, a_all, b_all, a_send, a_recv, b_send, b_recv):
    rows, cols = lax.axis_size("row"), lax.axis_size("col")
    r, c = lax.axis_index("row"), lax.axis_index("col")
    half = cols // 2
    dest = 2 * r + c // half
    slot = c % half
    source_row = c // 2
    source_col = c % 2 * half
    barrier = pltpu.get_barrier_semaphore()
    for k in range(1, cols):
        pl.semaphore_signal(
            barrier, inc=1, device_id=(r, (c + k) % cols), device_id_type=MESH
        )
    for k in range(rows):

        @pl.when(jnp.logical_or(k != 0, dest != c))
        def _(k=k):
            pl.semaphore_signal(
                barrier, inc=1, device_id=((r + k) % rows, dest), device_id_type=MESH
            )

    for d in range(half):

        @pl.when(jnp.logical_or(source_row != r, source_col + d != c))
        def _(d=d):
            pl.semaphore_signal(
                barrier, inc=1, device_id=(source_row, source_col + d), device_id_type=MESH
            )

    own = jnp.where(dest == c, 1, 0)
    pl.semaphore_wait(barrier, cols - 1 + rows + half - 2 * own)

    def a_copy(k):
        return pltpu.make_async_remote_copy(
            src_ref=a_ref,
            dst_ref=a_all.at[c],
            send_sem=a_send.at[k],
            recv_sem=a_recv.at[c],
            device_id=(r, (c + k) % cols),
            device_id_type=MESH,
        )

    def b_copy(k):
        return pltpu.make_async_remote_copy(
            src_ref=b_ref,
            dst_ref=b_all.at[slot],
            send_sem=b_send.at[k],
            recv_sem=b_recv.at[slot],
            device_id=((r + k) % rows, dest),
            device_id_type=MESH,
        )

    def landed(ref, sem):
        return pltpu.make_async_remote_copy(
            src_ref=ref,
            dst_ref=ref,
            send_sem=sem,
            recv_sem=sem,
            device_id=(r, c),
            device_id_type=MESH,
        )

    for k in range(max(cols, rows)):
        if 0 < k < rows:
            b_copy(k).start()
        if k == 0:

            @pl.when(dest != c)
            def _():
                b_copy(0).start()

        if k > 0:
            a_copy(k).start()
    a_all[c] = a_ref[...]

    @pl.when(dest == c)
    def _():
        b_all[slot] = b_ref[...]

    for k in range(1, cols):
        a_copy(k).wait_send()
    for k in range(1, rows):
        b_copy(k).wait_send()

    @pl.when(dest != c)
    def _():
        b_copy(0).wait_send()

    for k in range(1, cols):
        origin = (c + k) % cols
        landed(a_all.at[origin], a_recv.at[origin]).wait_recv()
    for d in range(half):

        @pl.when(jnp.logical_or(source_row != r, source_col + d != c))
        def _(d=d):
            landed(b_all.at[d], b_recv.at[d]).wait_recv()


def run_spread(a_block, b_block, rows, cols):
    half = cols // 2
    return pl.pallas_call(
        spread_factors,
        in_specs=[FULL, FULL],
        out_specs=[FULL, FULL],
        out_shape=[
            jax.ShapeDtypeStruct((cols,) + a_block.shape, jnp.bfloat16),
            jax.ShapeDtypeStruct((half,) + b_block.shape, jnp.bfloat16),
        ],
        scratch_shapes=[
            pltpu.SemaphoreType.DMA((cols,)),
            pltpu.SemaphoreType.DMA((cols,)),
            pltpu.SemaphoreType.DMA((rows,)),
            pltpu.SemaphoreType.DMA((half,)),
        ],
        compiler_params=pltpu.CompilerParams(collective_id=0, has_side_effects=True),
        name="spread_factors",
    )(a_block, b_block)


def pair_tile(
    pos_ref,
    a_ref,
    b_ref,
    offset_ref,
    project_ref,
    expand_ref,
    shrink_ref,
    bins_ref,
    pair_ref,
    logit_ref,
    c_scr,
    x_scr,
    right_scr,
):
    step = pl.program_id(0)
    seqs = b_ref.shape[2]

    @pl.when(step == 0)
    def _():
        for d in range(8):
            right_scr[4 * d : 4 * d + 4, :] = b_ref[d, 128:, :128].astype(jnp.float32)[:4]

    factors = jnp.concatenate([a_ref[0, :seqs, :], a_ref[1, :seqs, :]], axis=1)
    outer = mm(b_ref[:, :128, :].reshape(1024, seqs), factors)
    c_scr[0] = outer[:, :128]
    c_scr[1] = outer[:, 128:]
    lane = lax.broadcasted_iota(jnp.int32, (32, 128), 1)
    low = lane < 64
    even = lane % 64 < 32
    for part in range(2):
        for e in range(0, 32, 4):
            y = [c_scr[part, pl.ds(e + k, 32, stride=32), :] for k in range(4)]
            u = [
                jnp.where(low, y[0], pltpu.roll(y[2], 64, 1)),
                jnp.where(low, y[1], pltpu.roll(y[3], 64, 1)),
                jnp.where(low, pltpu.roll(y[0], 64, 1), y[2]),
                jnp.where(low, pltpu.roll(y[1], 64, 1), y[3]),
            ]
            z = [
                jnp.where(even, u[0], pltpu.roll(u[1], 32, 1)),
                jnp.where(even, pltpu.roll(u[0], 96, 1), u[1]),
                jnp.where(even, u[2], pltpu.roll(u[3], 32, 1)),
                jnp.where(even, pltpu.roll(u[2], 96, 1), u[3]),
            ]
            for i in range(4):
                row = (part * 4 + i) * 32
                x_scr[row : row + 32, e * 32 : e * 32 + 128] = (z[i] * (1.0 / seqs)).astype(
                    jnp.bfloat16
                )
    projected = mm(x_scr[...], project_ref[...])
    index = lax.broadcasted_iota(jnp.int32, (256, 128), 0)
    bins = lax.broadcasted_iota(jnp.int32, (256, 128), 1)
    offset = (pos_ref[1] + index % 32) - (pos_ref[0] + step * 8 + index // 32)
    onehot = jnp.where(jnp.clip(offset, -CLIP, CLIP) + CLIP == bins, 1.0, 0.0)
    relative = mm(onehot.astype(jnp.bfloat16), offset_ref[...])
    left0 = a_ref[0, seqs:, :].astype(jnp.float32)
    left1 = a_ref[1, seqs:, :].astype(jnp.float32)
    left = [left0[i : i + 1] for i in range(4)] + [left1[i : i + 1] for i in range(4)]
    right = right_scr[...]
    embedded = jnp.concatenate([right + one for one in left], axis=0)
    start = embedded + relative + projected
    hidden = jnp.maximum(
        mm(standardize_features(start).astype(jnp.bfloat16), expand_ref[...]), 0.0
    ).astype(jnp.bfloat16)
    final = (start + mm(hidden, shrink_ref[...])).astype(jnp.bfloat16)
    pair_ref[...] = final.reshape(8, 32, 128)
    logit_ref[...] = mm(final, bins_ref[...]).reshape(8, 32, 64)


def run_pair(pos, a_all, b_all, offset, project, expand, shrink, bins):
    seqs = b_all.shape[2]
    return pl.pallas_call(
        pair_tile,
        grid=(8,),
        in_specs=[
            pl.BlockSpec(memory_space=pltpu.SMEM),
            pl.BlockSpec((2,) + a_all.shape[1:], lambda i: (i, 0, 0)),
        ]
        + [FULL] * 6,
        out_specs=[
            pl.BlockSpec((8, 32, 128), lambda i: (i, 0, 0)),
            pl.BlockSpec((8, 32, 64), lambda i: (i, 0, 0)),
        ],
        out_shape=[
            jax.ShapeDtypeStruct((64, 32, 128), jnp.bfloat16),
            jax.ShapeDtypeStruct((64, 32, 64), jnp.float32),
        ],
        scratch_shapes=[
            pltpu.VMEM((2, 1024, 128), jnp.float32),
            pltpu.VMEM((256, 1024), jnp.bfloat16),
            pltpu.VMEM((32, 128), jnp.float32),
        ],
        compiler_params=pltpu.CompilerParams(
            dimension_semantics=("arbitrary",), vmem_limit_bytes=48 * 1024 * 1024
        ),
        name="pair_tile",
    )(pos, a_all, b_all, offset, project, expand, shrink, bins)


def shards(
    homolog_stack,
    per_amino_features,
    asking_matrix,
    lookup_matrix,
    content_matrix,
    sigmoid_scaling_matrix,
    attention_result_matrix,
    stack_transition_expand_matrix,
    stack_transition_shrink_matrix,
    former_factor_matrix,
    latter_factor_matrix,
    factor_mean_projection,
    row_amino_embedding,
    column_amino_embedding,
    offset_embedding_matrix,
    grid_transition_expand,
    grid_transition_shrink,
    distance_bins_matrix,
):
    rows = lax.axis_size("row")
    cols = lax.axis_size("col")
    whole = rows * cols
    seq_here, residues, width = homolog_stack.shape
    res_here = residues // whole
    fragments = homolog_stack.reshape(1, seq_here, whole, res_here, width)
    moved = lax.all_to_all(fragments, ("row", "col"), split_axis=2, concat_axis=0, tiled=True)
    local = moved.reshape(-1, res_here, width)
    seqs = local.shape[0]
    both = jnp.concatenate(
        [jnp.tile(former_factor_matrix, (1, 4)), jnp.tile(latter_factor_matrix, (1, 4))], axis=1
    )
    updated, a_block, b_block = run_attention(
        local.transpose(1, 0, 2),
        jnp.pad(per_amino_features, ((0, 12), (0, 0))),
        (
            asking_matrix,
            lookup_matrix,
            content_matrix,
            sigmoid_scaling_matrix,
            attention_result_matrix,
            stack_transition_expand_matrix,
            stack_transition_shrink_matrix,
            both,
            row_amino_embedding,
            column_amino_embedding,
        ),
    )
    alignment_output = updated.reshape(seqs, res_here, width)
    a_all, b_all = run_spread(a_block, b_block, rows, cols)
    r, c = lax.axis_index("row"), lax.axis_index("col")
    factor = former_factor_matrix.shape[1]
    project = (
        factor_mean_projection.reshape(factor, factor, -1)
        .transpose(1, 0, 2)
        .reshape(factor * factor, -1)
    )
    row_len, col_len = residues // rows, residues // cols
    pos = jnp.stack([r * row_len, c * col_len]).astype(jnp.int32)
    pair_output, logits = run_pair(
        pos,
        a_all,
        b_all,
        jnp.pad(offset_embedding_matrix, ((0, 127 - 2 * CLIP), (0, 0))),
        project,
        grid_transition_expand,
        grid_transition_shrink,
        distance_bins_matrix,
    )
    rounded = logits.astype(jnp.bfloat16)
    mirrors = []
    for k in range(2):
        pairs = []
        for rr in range(rows):
            for cc in range(cols):
                pairs.append((rr * cols + cc, cc // 2 * cols + 2 * rr + (cc % 2 ^ k)))
        half = lax.dynamic_slice_in_dim(rounded, (c % 2 ^ k) * col_len, col_len, 0)
        mirrors.append(lax.ppermute(half, ("row", "col"), pairs))
    flip = c % 2 == 0
    first = jnp.where(flip, mirrors[0], mirrors[1])
    second = jnp.where(flip, mirrors[1], mirrors[0])
    mirror = jnp.concatenate([first, second], axis=1)
    distogram = (logits + mirror.transpose(1, 0, 2).astype(jnp.float32)).astype(jnp.bfloat16)
    return (alignment_output, pair_output, distogram)


def solution(mesh):
    placed = (P(("row", "col"), None, None), P(("row", "col"), None)) + (P(),) * 16
    return jax.shard_map(
        shards,
        mesh=mesh,
        in_specs=placed,
        out_specs=(P(None, ("row", "col"), None), P("row", "col", None), P("row", "col", None)),
        check_vma=False,
    )
```

```python
import functools
import math

import jax
import jax.numpy as jnp
from jax import lax
from jax.experimental import pallas as pl
from jax.experimental.pallas import tpu as pltpu
from jax.sharding import PartitionSpec as P

HEADS = 8
HEAD = 32
CLIP = 32
MESH = pl.DeviceIdType.MESH
FULL = pl.BlockSpec(memory_space=pltpu.VMEM)


def standardize_features(values):
    middle = jnp.mean(values, -1, keepdims=True)
    centred = values - middle
    spread = jnp.mean(centred * centred, -1, keepdims=True)
    return centred * lax.rsqrt(spread + 1e-05)


def resident(shape):
    return pl.BlockSpec(shape, lambda i: (0,) * len(shape))


def mm(a, b):
    return jnp.dot(a, b, preferred_element_type=jnp.float32)


def column_attention(
    x_ref,
    feat_ref,
    wq_ref,
    wk_ref,
    wv_ref,
    wg_ref,
    wo_ref,
    we_ref,
    ws_ref,
    factor_ref,
    row_ref,
    column_ref,
    out_ref,
    a_ref,
    b_ref,
    q_scr,
    kt_scr,
    v_scr,
    acc_scr,
    fac_scr,
):
    step = pl.program_id(0)
    seqs = x_ref.shape[1]
    x = x_ref[0].astype(jnp.float32)
    normed = standardize_features(x).astype(jnp.bfloat16)
    q_scr[...] = mm(normed, wq_ref[...]).astype(jnp.bfloat16)
    kt_scr[...] = mm(normed, wk_ref[...]).T.astype(jnp.bfloat16)
    v = mm(normed, wv_ref[...]).astype(jnp.bfloat16)
    ones = jnp.ones((seqs, 128), jnp.bfloat16)
    v_scr[0] = jnp.concatenate([v[:, :128], ones], axis=1)
    v_scr[1] = jnp.concatenate([v[:, 128:], ones], axis=1)
    acc_scr[...] = jnp.zeros_like(acc_scr)
    lane = lax.broadcasted_iota(jnp.int32, (seqs, 256), 1)
    factor = math.log2(math.e) / math.sqrt(HEAD)

    def one_head(h, carry):
        group = h // 4
        q = jnp.where(lane // HEAD == h, q_scr[...], jnp.zeros((), jnp.bfloat16))
        scores = mm(q, kt_scr[...])
        top = jnp.max(scores, axis=-1, keepdims=True)
        weights = jnp.exp2((scores - top) * factor).astype(jnp.bfloat16)
        values = jnp.where(
            lane % 128 // HEAD == h % 4, v_scr[group], jnp.zeros((), jnp.bfloat16)
        )
        acc_scr[group] += mm(weights, values)
        return carry

    lax.fori_loop(0, HEADS, one_head, 0)
    attended = jnp.concatenate(
        [
            acc_scr[0, :, :128] / acc_scr[0, :, 128:],
            acc_scr[1, :, :128] / acc_scr[1, :, 128:],
        ],
        axis=1,
    )
    gate = jax.nn.sigmoid(mm(normed, wg_ref[...]))
    mixed = (attended * gate).astype(jnp.bfloat16)
    first = x + mm(mixed, wo_ref[...])
    hidden = jnp.maximum(
        mm(standardize_features(first).astype(jnp.bfloat16), we_ref[...]), 0.0
    ).astype(jnp.bfloat16)
    second = first + mm(hidden, ws_ref[...])
    out_ref[...] = second.astype(jnp.bfloat16)
    factors = mm(standardize_features(second).astype(jnp.bfloat16), factor_ref[...])
    fac_scr[...] = jnp.where(lane % 128 // HEAD == step, factors, fac_scr[...])

    @pl.when(step == pl.num_programs(0) - 1)
    def _():
        a_ref[:seqs, :] = fac_scr[:, :128].astype(jnp.bfloat16)
        b_ref[:128, :] = fac_scr[:, 128:].T.astype(jnp.bfloat16)
        feat = feat_ref[...]
        a_ref[seqs:, :] = mm(feat, row_ref[...]).astype(jnp.bfloat16)
        b_ref[128:, :128] = mm(feat, column_ref[...]).astype(jnp.bfloat16)
        b_ref[128:, 128:] = jnp.zeros((16, seqs - 128), jnp.bfloat16)


def run_attention(x, feat, weights, interpret=False):
    count_res, seqs, width = x.shape
    whole = [resident(one.shape) for one in (feat,) + weights]
    return pl.pallas_call(
        column_attention,
        grid=(count_res,),
        in_specs=[pl.BlockSpec((1, seqs, width), lambda i: (i, 0, 0))] + whole,
        out_specs=[
            pl.BlockSpec((seqs, width), lambda i: (0, i)),
            FULL,
            FULL,
        ],
        out_shape=[
            jax.ShapeDtypeStruct((seqs, count_res * width), jnp.bfloat16),
            jax.ShapeDtypeStruct((seqs + 16, 128), jnp.bfloat16),
            jax.ShapeDtypeStruct((144, seqs), jnp.bfloat16),
        ],
        scratch_shapes=[
            pltpu.VMEM((seqs, width), jnp.bfloat16),
            pltpu.VMEM((width, seqs), jnp.bfloat16),
            pltpu.VMEM((2, seqs, width), jnp.bfloat16),
            pltpu.VMEM((2, seqs, width), jnp.float32),
            pltpu.VMEM((seqs, width), jnp.float32),
        ],
        compiler_params=pltpu.CompilerParams(
            dimension_semantics=("arbitrary",), vmem_limit_bytes=48 * 1024 * 1024
        ),
        name="column_attention",
    )(x, feat, *weights)


def spread_factors(a_ref, b_ref, a_all, b_all, a_send, a_recv, b_send, b_recv):
    rows, cols = lax.axis_size("row"), lax.axis_size("col")
    half = cols // 2
    r, c = lax.axis_index("row"), lax.axis_index("col")
    high, within = c // half, c % half
    core = c % 2
    other_core = c + 1 - 2 * core
    other_high = (1 - high) * half + within
    other_row = r + 1 - 2 * (r % 2)
    ahead = 2 - 4 * core

    def along_x(column, shift):
        return column // half * half + (column % half + shift + half) % half

    def along_y(row, shift):
        return (row + shift + rows) % rows

    spot = within + 1 - 2 * (within % 2)
    first_dest = (spot, 2 * r + high)
    kept = other_row
    first_origin = (c // 2, c % 2 * half + kept)
    barrier = pltpu.get_barrier_semaphore()
    peers = [
        (r, other_core),
        (r, other_high),
        (r, along_x(c, 2)),
        (r, along_x(c, -2)),
        (other_row, c),
        (along_y(r, 2), c),
        (along_y(r, -2), c),
        first_dest,
        first_origin,
    ]
    for peer in peers:
        pl.semaphore_signal(barrier, inc=1, device_id=peer, device_id_type=MESH)
    pl.semaphore_wait(barrier, len(peers))
    sent = []

    def send(src, full, slot, sends, recvs, number, device):
        copy = pltpu.make_async_remote_copy(
            src_ref=src,
            dst_ref=full.at[slot],
            send_sem=sends.at[number],
            recv_sem=recvs.at[slot],
            device_id=device,
            device_id_type=MESH,
        )
        copy.start()
        sent.append(copy)

    def send_a(src, slot, number, column):
        send(src, a_all, slot, a_send, a_recv, number, (r, column))

    def send_b(src, slot, number, device):
        send(src, b_all, slot, b_send, b_recv, number, device)

    def arrived(full, slot, recvs):
        pltpu.make_async_remote_copy(
            src_ref=full.at[slot],
            dst_ref=full.at[slot],
            send_sem=recvs.at[slot],
            recv_sem=recvs.at[slot],
            device_id=(r, other_core),
            device_id_type=MESH,
        ).wait_recv()

    send_b(b_ref, within, 0, first_dest)
    send_a(a_ref, c, 0, other_high)
    send_a(a_ref, c, 1, along_x(c, ahead))
    send_a(a_ref, c, 2, along_x(c, -ahead))
    send_a(a_ref, c, 3, other_core)
    a_all[c] = a_ref[...]
    arrived(b_all, kept, b_recv)
    send_b(b_all.at[kept], kept, 1, (other_row, c))
    send_b(b_all.at[kept], kept, 2, (along_y(r, ahead), c))
    send_b(b_all.at[kept], kept, 3, (along_y(r, -ahead), c))
    arrived(a_all, other_high, a_recv)
    send_a(a_all.at[other_high], other_high, 4, along_x(c, ahead))
    send_a(a_all.at[other_high], other_high, 5, along_x(c, -ahead))
    send_a(a_all.at[other_high], other_high, 6, other_core)
    arrived(b_all, r, b_recv)
    send_b(b_all.at[r], r, 4, (along_y(r, ahead), c))
    send_b(b_all.at[r], r, 5, (along_y(r, -ahead), c))
    for turn, (a_slot, b_slot) in enumerate(((c, kept), (other_high, r))):
        back = along_x(a_slot, -ahead)
        arrived(a_all, back, a_recv)
        send_a(a_all.at[back], back, 7 + 4 * turn, along_x(c, ahead))
        send_a(a_all.at[back], back, 8 + 4 * turn, other_core)
        behind = along_y(b_slot, -ahead)
        arrived(b_all, behind, b_recv)
        send_b(b_all.at[behind], behind, 6 + turn, (along_y(r, ahead), c))
        front = along_x(a_slot, ahead)
        arrived(a_all, front, a_recv)
        send_a(a_all.at[front], front, 9 + 4 * turn, other_core)
    for turn, a_slot in enumerate((c, other_high)):
        far = along_x(a_slot, 4)
        arrived(a_all, far, a_recv)
        send_a(a_all.at[far], far, 10 + 4 * turn, other_core)
    for b_slot in (kept, r):
        arrived(b_all, along_y(b_slot, ahead), b_recv)
        arrived(b_all, along_y(b_slot, 4), b_recv)
    for a_slot in (c, other_high):
        mate = a_slot + 1 - 2 * core
        for shift in range(0, half, 2):
            arrived(a_all, along_x(mate, shift), a_recv)
    for copy in sent:
        copy.wait_send()


def run_spread(a_block, b_block, rows, cols):
    half = cols // 2
    return pl.pallas_call(
        spread_factors,
        in_specs=[FULL, FULL],
        out_specs=[FULL, FULL],
        out_shape=[
            jax.ShapeDtypeStruct((cols,) + a_block.shape, jnp.bfloat16),
            jax.ShapeDtypeStruct((half,) + b_block.shape, jnp.bfloat16),
        ],
        scratch_shapes=[
            pltpu.SemaphoreType.DMA((15,)),
            pltpu.SemaphoreType.DMA((cols,)),
            pltpu.SemaphoreType.DMA((8,)),
            pltpu.SemaphoreType.DMA((half,)),
        ],
        compiler_params=pltpu.CompilerParams(collective_id=0, has_side_effects=True),
        name="spread_factors",
    )(a_block, b_block)


def pair_tile(
    pos_ref,
    a_ref,
    b_ref,
    offset_ref,
    project_ref,
    expand_ref,
    shrink_ref,
    bins_ref,
    pair_ref,
    logit_ref,
    c_scr,
    x_scr,
    right_scr,
):
    step = pl.program_id(0)
    seqs = b_ref.shape[2]

    @pl.when(step == 0)
    def _():
        for d in range(8):
            right_scr[4 * d : 4 * d + 4, :] = b_ref[d, 128:, :128].astype(jnp.float32)[:4]

    factors = jnp.concatenate([a_ref[2 * step, :seqs, :], a_ref[2 * step + 1, :seqs, :]], axis=1)
    outer = mm(b_ref[:, :128, :].reshape(1024, seqs), factors)
    c_scr[0] = outer[:, :128]
    c_scr[1] = outer[:, 128:]
    lane = lax.broadcasted_iota(jnp.int32, (32, 128), 1)
    low = lane < 64
    even = lane % 64 < 32
    for part in range(2):
        for e in range(0, 32, 4):
            y = [c_scr[part, pl.ds(e + k, 32, stride=32), :] for k in range(4)]
            u = [
                jnp.where(low, y[0], pltpu.roll(y[2], 64, 1)),
                jnp.where(low, y[1], pltpu.roll(y[3], 64, 1)),
                jnp.where(low, pltpu.roll(y[0], 64, 1), y[2]),
                jnp.where(low, pltpu.roll(y[1], 64, 1), y[3]),
            ]
            z = [
                jnp.where(even, u[0], pltpu.roll(u[1], 32, 1)),
                jnp.where(even, pltpu.roll(u[0], 96, 1), u[1]),
                jnp.where(even, u[2], pltpu.roll(u[3], 32, 1)),
                jnp.where(even, pltpu.roll(u[2], 96, 1), u[3]),
            ]
            for i in range(4):
                row = (part * 4 + i) * 32
                x_scr[row : row + 32, e * 32 : e * 32 + 128] = (z[i] * (1.0 / seqs)).astype(
                    jnp.bfloat16
                )
    projected = mm(x_scr[...], project_ref[...])
    index = lax.broadcasted_iota(jnp.int32, (256, 128), 0)
    bins = lax.broadcasted_iota(jnp.int32, (256, 128), 1)
    offset = (pos_ref[1] + index % 32) - (pos_ref[0] + step * 8 + index // 32)
    onehot = jnp.where(jnp.clip(offset, -CLIP, CLIP) + CLIP == bins, 1.0, 0.0)
    relative = mm(onehot.astype(jnp.bfloat16), offset_ref[...])
    left0 = a_ref[2 * step, seqs:, :].astype(jnp.float32)
    left1 = a_ref[2 * step + 1, seqs:, :].astype(jnp.float32)
    left = [left0[i : i + 1] for i in range(4)] + [left1[i : i + 1] for i in range(4)]
    right = right_scr[...]
    embedded = jnp.concatenate([right + one for one in left], axis=0)
    start = embedded + relative + projected
    hidden = jnp.maximum(
        mm(standardize_features(start).astype(jnp.bfloat16), expand_ref[...]), 0.0
    ).astype(jnp.bfloat16)
    final = (start + mm(hidden, shrink_ref[...])).astype(jnp.bfloat16)
    pair_ref[...] = final.reshape(8, 32, 128)
    logit_ref[...] = mm(final, bins_ref[...]).reshape(8, 32, 64)


def run_pair(pos, a_all, b_all, offset, project, expand, shrink, bins):
    seqs = b_all.shape[2]
    return pl.pallas_call(
        pair_tile,
        grid=(8,),
        in_specs=[
            pl.BlockSpec(memory_space=pltpu.SMEM),
            FULL,
            FULL,
        ]
        + [resident(one.shape) for one in (offset, project, expand, shrink, bins)],
        out_specs=[
            pl.BlockSpec((8, 32, 128), lambda i: (i, 0, 0)),
            pl.BlockSpec((8, 32, 64), lambda i: (i, 0, 0)),
        ],
        out_shape=[
            jax.ShapeDtypeStruct((64, 32, 128), jnp.bfloat16),
            jax.ShapeDtypeStruct((64, 32, 64), jnp.float32),
        ],
        scratch_shapes=[
            pltpu.VMEM((2, 1024, 128), jnp.float32),
            pltpu.VMEM((256, 1024), jnp.bfloat16),
            pltpu.VMEM((32, 128), jnp.float32),
        ],
        compiler_params=pltpu.CompilerParams(
            dimension_semantics=("arbitrary",), vmem_limit_bytes=48 * 1024 * 1024
        ),
        name="pair_tile",
    )(pos, a_all, b_all, offset, project, expand, shrink, bins)


def shards(
    homolog_stack,
    per_amino_features,
    asking_matrix,
    lookup_matrix,
    content_matrix,
    sigmoid_scaling_matrix,
    attention_result_matrix,
    stack_transition_expand_matrix,
    stack_transition_shrink_matrix,
    former_factor_matrix,
    latter_factor_matrix,
    factor_mean_projection,
    row_amino_embedding,
    column_amino_embedding,
    offset_embedding_matrix,
    grid_transition_expand,
    grid_transition_shrink,
    distance_bins_matrix,
):
    rows = lax.axis_size("row")
    cols = lax.axis_size("col")
    whole = rows * cols
    seq_here, residues, width = homolog_stack.shape
    res_here = residues // whole
    fragments = homolog_stack.reshape(1, seq_here, whole, res_here, width)
    moved = lax.all_to_all(fragments, ("row", "col"), split_axis=2, concat_axis=0, tiled=True)
    local = moved.reshape(-1, res_here, width)
    seqs = local.shape[0]
    both = jnp.concatenate(
        [jnp.tile(former_factor_matrix, (1, 4)), jnp.tile(latter_factor_matrix, (1, 4))], axis=1
    )
    updated, a_block, b_block = run_attention(
        local.transpose(1, 0, 2),
        jnp.pad(per_amino_features, ((0, 12), (0, 0))),
        (
            asking_matrix,
            lookup_matrix,
            content_matrix,
            sigmoid_scaling_matrix,
            attention_result_matrix,
            stack_transition_expand_matrix,
            stack_transition_shrink_matrix,
            both,
            row_amino_embedding,
            column_amino_embedding,
        ),
    )
    alignment_output = updated.reshape(seqs, res_here, width)
    a_all, b_all = run_spread(a_block, b_block, rows, cols)
    r, c = lax.axis_index("row"), lax.axis_index("col")
    factor = former_factor_matrix.shape[1]
    project = (
        factor_mean_projection.reshape(factor, factor, -1)
        .transpose(1, 0, 2)
        .reshape(factor * factor, -1)
    )
    row_len, col_len = residues // rows, residues // cols
    pos = jnp.stack([r * row_len, c * col_len]).astype(jnp.int32)
    pair_output, logits = run_pair(
        pos,
        a_all,
        b_all,
        jnp.pad(offset_embedding_matrix, ((0, 127 - 2 * CLIP), (0, 0))),
        project,
        grid_transition_expand,
        grid_transition_shrink,
        distance_bins_matrix,
    )
    rounded = logits.astype(jnp.bfloat16)
    mirrors = []
    for k in range(2):
        pairs = []
        for rr in range(rows):
            for cc in range(cols):
                pairs.append((rr * cols + cc, cc // 2 * cols + 2 * rr + (cc % 2 ^ k)))
        half = lax.dynamic_slice_in_dim(rounded, (c % 2 ^ k) * col_len, col_len, 0)
        mirrors.append(lax.ppermute(half, ("row", "col"), pairs))
    flip = c % 2 == 0
    first = jnp.where(flip, mirrors[0], mirrors[1])
    second = jnp.where(flip, mirrors[1], mirrors[0])
    mirror = jnp.concatenate([first, second], axis=1)
    distogram = (logits + mirror.transpose(1, 0, 2).astype(jnp.float32)).astype(jnp.bfloat16)
    return (alignment_output, pair_output, distogram)


def solution(mesh):
    placed = (P(("row", "col"), None, None), P(("row", "col"), None)) + (P(),) * 16
    return jax.shard_map(
        shards,
        mesh=mesh,
        in_specs=placed,
        out_specs=(P(None, ("row", "col"), None), P("row", "col", None), P("row", "col", None)),
        check_vma=False,
    )
```

```python
import functools
import math

import jax
import jax.numpy as jnp
from jax import lax
from jax.experimental import pallas as pl
from jax.experimental.pallas import tpu as pltpu
from jax.sharding import PartitionSpec as P

HEADS = 8
HEAD = 32
CLIP = 32
VMEM_LIMIT = 67043328
MESH = pl.DeviceIdType.MESH
FULL = pl.BlockSpec(memory_space=pltpu.VMEM)


def standardize_features(values):
    middle = jnp.mean(values, -1, keepdims=True)
    centred = values - middle
    spread = jnp.mean(centred * centred, -1, keepdims=True)
    return centred * lax.rsqrt(spread + 1e-05)


def resident(shape):
    return pl.BlockSpec(shape, lambda i: (0,) * len(shape))


def mm(a, b):
    return jnp.dot(a, b, preferred_element_type=jnp.float32)


def column_attention(
    x_ref,
    feat_ref,
    wq_ref,
    wk_ref,
    wv_ref,
    wg_ref,
    wo_ref,
    we_ref,
    ws_ref,
    factor_ref,
    row_ref,
    column_ref,
    out_ref,
    a_ref,
    b_ref,
    q_scr,
    kt_scr,
    v_scr,
    acc_scr,
    fac_scr,
):
    step = pl.program_id(0)
    seqs = x_ref.shape[1]
    x = x_ref[0].astype(jnp.float32)
    normed = standardize_features(x).astype(jnp.bfloat16)
    q_scr[...] = mm(normed, wq_ref[...]).astype(jnp.bfloat16)
    kt_scr[...] = mm(normed, wk_ref[...]).T.astype(jnp.bfloat16)
    v = mm(normed, wv_ref[...]).astype(jnp.bfloat16)
    ones = jnp.ones((seqs, 128), jnp.bfloat16)
    v_scr[0] = jnp.concatenate([v[:, :128], ones], axis=1)
    v_scr[1] = jnp.concatenate([v[:, 128:], ones], axis=1)
    acc_scr[...] = jnp.zeros_like(acc_scr)
    lane = lax.broadcasted_iota(jnp.int32, (seqs, 256), 1)
    factor = math.log2(math.e) / math.sqrt(HEAD)

    def one_head(h, carry):
        group = h // 4
        q = jnp.where(lane // HEAD == h, q_scr[...], jnp.zeros((), jnp.bfloat16))
        scores = mm(q, kt_scr[...])
        top = jnp.max(scores, axis=-1, keepdims=True)
        weights = jnp.exp2((scores - top) * factor).astype(jnp.bfloat16)
        values = jnp.where(
            lane % 128 // HEAD == h % 4, v_scr[group], jnp.zeros((), jnp.bfloat16)
        )
        acc_scr[group] += mm(weights, values)
        return carry

    lax.fori_loop(0, HEADS, one_head, 0)
    attended = jnp.concatenate(
        [
            acc_scr[0, :, :128] / acc_scr[0, :, 128:],
            acc_scr[1, :, :128] / acc_scr[1, :, 128:],
        ],
        axis=1,
    )
    gate = jax.nn.sigmoid(mm(normed, wg_ref[...]))
    mixed = (attended * gate).astype(jnp.bfloat16)
    first = x + mm(mixed, wo_ref[...])
    hidden = jnp.maximum(
        mm(standardize_features(first).astype(jnp.bfloat16), we_ref[...]), 0.0
    ).astype(jnp.bfloat16)
    second = first + mm(hidden, ws_ref[...])
    out_ref[...] = second.astype(jnp.bfloat16)
    factors = mm(standardize_features(second).astype(jnp.bfloat16), factor_ref[...])
    fac_scr[...] = jnp.where(lane % 128 // HEAD == step, factors, fac_scr[...])

    @pl.when(step == pl.num_programs(0) - 1)
    def _():
        a_ref[:seqs, :] = fac_scr[:, :128].astype(jnp.bfloat16)
        b_ref[:128, :] = fac_scr[:, 128:].T.astype(jnp.bfloat16)
        feat = feat_ref[...]
        a_ref[seqs:, :] = mm(feat, row_ref[...]).astype(jnp.bfloat16)
        b_ref[128:, :128] = mm(feat, column_ref[...]).astype(jnp.bfloat16)
        b_ref[128:, 128:] = jnp.zeros((16, seqs - 128), jnp.bfloat16)


def run_attention(x, feat, weights, interpret=False):
    count_res, seqs, width = x.shape
    whole = [resident(one.shape) for one in (feat,) + weights]
    return pl.pallas_call(
        column_attention,
        grid=(count_res,),
        in_specs=[pl.BlockSpec((1, seqs, width), lambda i: (i, 0, 0))] + whole,
        out_specs=[
            pl.BlockSpec((seqs, width), lambda i: (0, i)),
            FULL,
            FULL,
        ],
        out_shape=[
            jax.ShapeDtypeStruct((seqs, count_res * width), jnp.bfloat16),
            jax.ShapeDtypeStruct((seqs + 16, 128), jnp.bfloat16),
            jax.ShapeDtypeStruct((144, seqs), jnp.bfloat16),
        ],
        scratch_shapes=[
            pltpu.VMEM((seqs, width), jnp.bfloat16),
            pltpu.VMEM((width, seqs), jnp.bfloat16),
            pltpu.VMEM((2, seqs, width), jnp.bfloat16),
            pltpu.VMEM((2, seqs, width), jnp.float32),
            pltpu.VMEM((seqs, width), jnp.float32),
        ],
        compiler_params=pltpu.CompilerParams(
            dimension_semantics=("arbitrary",), vmem_limit_bytes=VMEM_LIMIT
        ),
        name="column_attention",
    )(x, feat, *weights)


def spread_factors(a_ref, b_ref, a_all, b_all, a_send, a_recv, b_send, b_recv):
    rows, cols = lax.axis_size("row"), lax.axis_size("col")
    half = cols // 2
    r, c = lax.axis_index("row"), lax.axis_index("col")
    high, within = c // half, c % half
    core = c % 2
    other_core = c + 1 - 2 * core
    other_high = (1 - high) * half + within
    other_row = r + 1 - 2 * (r % 2)
    ahead = 2 - 4 * core

    def along_x(column, shift):
        return column // half * half + (column % half + shift + half) % half

    def along_y(row, shift):
        return (row + shift + rows) % rows

    spot = within + 1 - 2 * (within % 2)
    first_dest = (spot, 2 * r + high)
    kept = other_row
    first_origin = (c // 2, c % 2 * half + kept)
    barrier = pltpu.get_barrier_semaphore()
    peers = [
        (r, other_core),
        (r, other_high),
        (r, along_x(c, 2)),
        (r, along_x(c, -2)),
        (other_row, c),
        (along_y(r, 2), c),
        (along_y(r, -2), c),
        first_dest,
        first_origin,
    ]
    for peer in peers:
        pl.semaphore_signal(barrier, inc=1, device_id=peer, device_id_type=MESH)
    pl.semaphore_wait(barrier, len(peers))
    sent = []

    def send(src, full, slot, sends, recvs, number, device):
        copy = pltpu.make_async_remote_copy(
            src_ref=src,
            dst_ref=full.at[slot],
            send_sem=sends.at[number],
            recv_sem=recvs.at[slot],
            device_id=device,
            device_id_type=MESH,
        )
        copy.start()
        sent.append(copy)

    def send_a(src, slot, number, column):
        send(src, a_all, slot, a_send, a_recv, number, (r, column))

    def send_b(src, slot, number, device):
        send(src, b_all, slot, b_send, b_recv, number, device)

    def arrived(full, slot, recvs):
        pltpu.make_async_remote_copy(
            src_ref=full.at[slot],
            dst_ref=full.at[slot],
            send_sem=recvs.at[slot],
            recv_sem=recvs.at[slot],
            device_id=(r, other_core),
            device_id_type=MESH,
        ).wait_recv()

    send_b(b_ref, within, 0, first_dest)
    send_a(a_ref, c, 0, other_high)
    send_a(a_ref, c, 1, along_x(c, ahead))
    send_a(a_ref, c, 2, along_x(c, -ahead))
    send_a(a_ref, c, 3, other_core)
    a_all[c] = a_ref[...]
    arrived(b_all, kept, b_recv)
    send_b(b_all.at[kept], kept, 1, (other_row, c))
    send_b(b_all.at[kept], kept, 2, (along_y(r, ahead), c))
    send_b(b_all.at[kept], kept, 3, (along_y(r, -ahead), c))
    arrived(a_all, other_high, a_recv)
    send_a(a_all.at[other_high], other_high, 4, along_x(c, ahead))
    send_a(a_all.at[other_high], other_high, 5, along_x(c, -ahead))
    send_a(a_all.at[other_high], other_high, 6, other_core)
    arrived(b_all, r, b_recv)
    send_b(b_all.at[r], r, 4, (along_y(r, ahead), c))
    send_b(b_all.at[r], r, 5, (along_y(r, -ahead), c))
    for turn, (a_slot, b_slot) in enumerate(((c, kept), (other_high, r))):
        back = along_x(a_slot, -ahead)
        arrived(a_all, back, a_recv)
        send_a(a_all.at[back], back, 7 + 4 * turn, along_x(c, ahead))
        send_a(a_all.at[back], back, 8 + 4 * turn, other_core)
        behind = along_y(b_slot, -ahead)
        arrived(b_all, behind, b_recv)
        send_b(b_all.at[behind], behind, 6 + turn, (along_y(r, ahead), c))
        front = along_x(a_slot, ahead)
        arrived(a_all, front, a_recv)
        send_a(a_all.at[front], front, 9 + 4 * turn, other_core)
    for turn, a_slot in enumerate((c, other_high)):
        far = along_x(a_slot, 4)
        arrived(a_all, far, a_recv)
        send_a(a_all.at[far], far, 10 + 4 * turn, other_core)
    for b_slot in (kept, r):
        arrived(b_all, along_y(b_slot, ahead), b_recv)
        arrived(b_all, along_y(b_slot, 4), b_recv)
    for a_slot in (c, other_high):
        mate = a_slot + 1 - 2 * core
        for shift in range(0, half, 2):
            arrived(a_all, along_x(mate, shift), a_recv)
    for copy in sent:
        copy.wait_send()


def run_spread(a_block, b_block, rows, cols):
    half = cols // 2
    return pl.pallas_call(
        spread_factors,
        in_specs=[FULL, FULL],
        out_specs=[FULL, FULL],
        out_shape=[
            jax.ShapeDtypeStruct((cols,) + a_block.shape, jnp.bfloat16),
            jax.ShapeDtypeStruct((half,) + b_block.shape, jnp.bfloat16),
        ],
        scratch_shapes=[
            pltpu.SemaphoreType.DMA((15,)),
            pltpu.SemaphoreType.DMA((cols,)),
            pltpu.SemaphoreType.DMA((8,)),
            pltpu.SemaphoreType.DMA((half,)),
        ],
        compiler_params=pltpu.CompilerParams(collective_id=0, has_side_effects=True),
        name="spread_factors",
    )(a_block, b_block)


def pair_tile(
    a_ref,
    b_ref,
    offset_ref,
    project_ref,
    expand_ref,
    shrink_ref,
    bins_ref,
    pair_ref,
    distogram_ref,
    c_scr,
    x_scr,
    right_scr,
    own_scr,
    out_scr,
    in_scr,
    turn_scr,
    send_sem,
    recv_sem,
):
    step = pl.program_id(0)
    seqs = b_ref.shape[2]
    r, c = lax.axis_index("row"), lax.axis_index("col")
    mirror_row, parity = c // 2, c % 2
    diagonal = mirror_row == r
    barrier = pltpu.get_barrier_semaphore()

    def mirror_copy(number):
        return pltpu.make_async_remote_copy(
            src_ref=out_scr.at[number],
            dst_ref=in_scr.at[parity, number % 4],
            send_sem=send_sem.at[number],
            recv_sem=recv_sem.at[parity, number % 4],
            device_id=(mirror_row, 2 * r + number // 4),
            device_id_type=MESH,
        )

    def stays(number):
        return jnp.logical_and(diagonal, number // 4 == parity)

    def dispatch(number):
        @pl.when(jnp.logical_not(stays(number)))
        def _():
            mirror_copy(number).start()

    @pl.when(step == 0)
    def _():
        for h in range(2):

            @pl.when(jnp.logical_not(jnp.logical_and(diagonal, parity == h)))
            def _(h=h):
                pl.semaphore_signal(
                    barrier, inc=1, device_id=(mirror_row, 2 * r + h), device_id_type=MESH
                )

    @pl.when(step == 1)
    def _():
        pl.semaphore_wait(barrier, 2 - jnp.where(diagonal, 1, 0))

    @pl.when(step == 0)
    def _():
        for d in range(8):
            right_scr[4 * d : 4 * d + 4, :] = b_ref[d, 128:, :128].astype(jnp.float32)[:4]

    factors = jnp.concatenate([a_ref[2 * step, :seqs, :], a_ref[2 * step + 1, :seqs, :]], axis=1)
    outer = mm(b_ref[:, :128, :].reshape(1024, seqs), factors)
    c_scr[0] = outer[:, :128]
    c_scr[1] = outer[:, 128:]

    @pl.when(step > 0)
    def _():
        dispatch(step - 1)

    lane = lax.broadcasted_iota(jnp.int32, (32, 128), 1)
    low = lane < 64
    even = lane % 64 < 32
    for part in range(2):
        for e in range(0, 32, 4):
            y = [c_scr[part, pl.ds(e + k, 32, stride=32), :] for k in range(4)]
            u = [
                jnp.where(low, y[0], pltpu.roll(y[2], 64, 1)),
                jnp.where(low, y[1], pltpu.roll(y[3], 64, 1)),
                jnp.where(low, pltpu.roll(y[0], 64, 1), y[2]),
                jnp.where(low, pltpu.roll(y[1], 64, 1), y[3]),
            ]
            z = [
                jnp.where(even, u[0], pltpu.roll(u[1], 32, 1)),
                jnp.where(even, pltpu.roll(u[0], 96, 1), u[1]),
                jnp.where(even, u[2], pltpu.roll(u[3], 32, 1)),
                jnp.where(even, pltpu.roll(u[2], 96, 1), u[3]),
            ]
            for i in range(4):
                row = (part * 4 + i) * 32
                x_scr[row : row + 32, e * 32 : e * 32 + 128] = (z[i] * (1.0 / seqs)).astype(
                    jnp.bfloat16
                )
    projected = mm(x_scr[...], project_ref[...])
    index = lax.broadcasted_iota(jnp.int32, (256, 128), 0)
    bins = lax.broadcasted_iota(jnp.int32, (256, 128), 1)
    offset = (c * 32 + index % 32) - (r * 64 + step * 8 + index // 32)
    onehot = jnp.where(jnp.clip(offset, -CLIP, CLIP) + CLIP == bins, 1.0, 0.0)
    relative = mm(onehot.astype(jnp.bfloat16), offset_ref[...])
    left0 = a_ref[2 * step, seqs:, :].astype(jnp.float32)
    left1 = a_ref[2 * step + 1, seqs:, :].astype(jnp.float32)
    left = [left0[i : i + 1] for i in range(4)] + [left1[i : i + 1] for i in range(4)]
    right = right_scr[...]
    embedded = jnp.concatenate([right + one for one in left], axis=0)
    start = embedded + relative + projected
    hidden = jnp.maximum(
        mm(standardize_features(start).astype(jnp.bfloat16), expand_ref[...]), 0.0
    ).astype(jnp.bfloat16)
    final = (start + mm(hidden, shrink_ref[...])).astype(jnp.bfloat16)
    pair_ref[...] = final.reshape(8, 32, 128)
    logits = mm(final, bins_ref[...])
    own_scr[step] = logits
    packed = jnp.where(bins[:128] < 64, logits[:128], logits[128:]).astype(jnp.bfloat16)
    out_scr[step] = packed

    @pl.when(stays(step))
    def _():
        in_scr[parity, step % 4] = packed

    @pl.when(step == pl.num_programs(0) - 1)
    def _():
        dispatch(step)
        for quarter in range(4):
            for k in range(2):

                @pl.when(jnp.logical_not(jnp.logical_and(diagonal, parity == k)))
                def _(k=k, quarter=quarter):
                    pltpu.make_async_remote_copy(
                        src_ref=in_scr.at[k, quarter],
                        dst_ref=in_scr.at[k, quarter],
                        send_sem=recv_sem.at[k, quarter],
                        recv_sem=recv_sem.at[k, quarter],
                        device_id=(mirror_row, 2 * r + k),
                        device_id_type=MESH,
                    ).wait_recv()

                for i in range(4):
                    rows = in_scr[k, quarter, 32 * i : 32 * i + 32, :].astype(jnp.float32)
                    first = k * 1024 + quarter * 8 + i
                    turn_scr[pl.ds(first, 32, stride=32), :] = rows
                    turn_scr[pl.ds(first + 4, 32, stride=32), :] = pltpu.roll(rows, 64, 1)
        for number in range(8):
            total = own_scr[number] + turn_scr[256 * number : 256 * number + 256, :]
            distogram_ref[8 * number : 8 * number + 8] = (
                total[:, :64].astype(jnp.bfloat16).reshape(8, 32, 64)
            )
        for number in range(8):

            @pl.when(jnp.logical_not(stays(number)))
            def _(number=number):
                mirror_copy(number).wait_send()


def run_pair(a_all, b_all, offset, project, expand, shrink, bins):
    return pl.pallas_call(
        pair_tile,
        grid=(8,),
        in_specs=[FULL, FULL]
        + [resident(one.shape) for one in (offset, project, expand, shrink, bins)],
        out_specs=[
            pl.BlockSpec((8, 32, 128), lambda i: (i, 0, 0)),
            pl.BlockSpec((64, 32, 64), lambda i: (0, 0, 0)),
        ],
        out_shape=[
            jax.ShapeDtypeStruct((64, 32, 128), jnp.bfloat16),
            jax.ShapeDtypeStruct((64, 32, 64), jnp.bfloat16),
        ],
        scratch_shapes=[
            pltpu.VMEM((2, 1024, 128), jnp.float32),
            pltpu.VMEM((256, 1024), jnp.bfloat16),
            pltpu.VMEM((32, 128), jnp.float32),
            pltpu.VMEM((8, 256, 128), jnp.float32),
            pltpu.VMEM((8, 128, 128), jnp.bfloat16),
            pltpu.VMEM((2, 4, 128, 128), jnp.bfloat16),
            pltpu.VMEM((2048, 128), jnp.float32),
            pltpu.SemaphoreType.DMA((8,)),
            pltpu.SemaphoreType.DMA((2, 4)),
        ],
        compiler_params=pltpu.CompilerParams(
            dimension_semantics=("arbitrary",),
            vmem_limit_bytes=VMEM_LIMIT,
            collective_id=1,
            has_side_effects=True,
        ),
        name="pair_tile",
    )(a_all, b_all, offset, project, expand, shrink, bins)


def shards(
    homolog_stack,
    per_amino_features,
    asking_matrix,
    lookup_matrix,
    content_matrix,
    sigmoid_scaling_matrix,
    attention_result_matrix,
    stack_transition_expand_matrix,
    stack_transition_shrink_matrix,
    former_factor_matrix,
    latter_factor_matrix,
    factor_mean_projection,
    row_amino_embedding,
    column_amino_embedding,
    offset_embedding_matrix,
    grid_transition_expand,
    grid_transition_shrink,
    distance_bins_matrix,
):
    rows = lax.axis_size("row")
    cols = lax.axis_size("col")
    whole = rows * cols
    seq_here, residues, width = homolog_stack.shape
    res_here = residues // whole
    fragments = homolog_stack.reshape(1, seq_here, whole, res_here, width)
    moved = lax.all_to_all(fragments, ("row", "col"), split_axis=2, concat_axis=0, tiled=True)
    local = moved.reshape(-1, res_here, width)
    seqs = local.shape[0]
    both = jnp.concatenate(
        [jnp.tile(former_factor_matrix, (1, 4)), jnp.tile(latter_factor_matrix, (1, 4))], axis=1
    )
    updated, a_block, b_block = run_attention(
        local.transpose(1, 0, 2),
        jnp.pad(per_amino_features, ((0, 12), (0, 0))),
        (
            asking_matrix,
            lookup_matrix,
            content_matrix,
            sigmoid_scaling_matrix,
            attention_result_matrix,
            stack_transition_expand_matrix,
            stack_transition_shrink_matrix,
            both,
            row_amino_embedding,
            column_amino_embedding,
        ),
    )
    alignment_output = updated.reshape(seqs, res_here, width)
    a_all, b_all = run_spread(a_block, b_block, rows, cols)
    factor = former_factor_matrix.shape[1]
    project = (
        factor_mean_projection.reshape(factor, factor, -1)
        .transpose(1, 0, 2)
        .reshape(factor * factor, -1)
    )
    pair_output, distogram = run_pair(
        a_all,
        b_all,
        jnp.pad(offset_embedding_matrix, ((0, 127 - 2 * CLIP), (0, 0))),
        project,
        grid_transition_expand,
        grid_transition_shrink,
        jnp.concatenate([distance_bins_matrix] * 2, axis=1),
    )
    return (alignment_output, pair_output, distogram)


def solution(mesh):
    placed = (P(("row", "col"), None, None), P(("row", "col"), None)) + (P(),) * 16
    return jax.shard_map(
        shards,
        mesh=mesh,
        in_specs=placed,
        out_specs=(P(None, ("row", "col"), None), P("row", "col", None), P("row", "col", None)),
        check_vma=False,
    )
```

```python
import functools
import math

import jax
import jax.numpy as jnp
from jax import lax
from jax.experimental import pallas as pl
from jax.experimental.pallas import tpu as pltpu
from jax.sharding import PartitionSpec as P

HEADS = 8
HEAD = 32
CLIP = 32
VMEM_LIMIT = 67043328
MESH = pl.DeviceIdType.MESH
FULL = pl.BlockSpec(memory_space=pltpu.VMEM)


def standardize_features(values):
    middle = jnp.mean(values, -1, keepdims=True)
    centred = values - middle
    spread = jnp.mean(centred * centred, -1, keepdims=True)
    return centred * lax.rsqrt(spread + 1e-05)


def resident(shape):
    return pl.BlockSpec(shape, lambda i: (0,) * len(shape))


def mm(a, b):
    return jnp.dot(a, b, preferred_element_type=jnp.float32)


def column_attention(
    x_ref,
    feat_ref,
    wq_ref,
    wk_ref,
    wv_ref,
    wg_ref,
    wo_ref,
    we_ref,
    ws_ref,
    factor_ref,
    row_ref,
    column_ref,
    out_ref,
    a_ref,
    b_ref,
    q_scr,
    kt_scr,
    v_scr,
    acc_scr,
    fac_scr,
):
    step = pl.program_id(0)
    seqs = x_ref.shape[1]
    x = x_ref[0].astype(jnp.float32)
    normed = standardize_features(x).astype(jnp.bfloat16)
    q_scr[...] = mm(normed, wq_ref[...]).astype(jnp.bfloat16)
    kt_scr[...] = mm(normed, wk_ref[...]).T.astype(jnp.bfloat16)
    v = mm(normed, wv_ref[...]).astype(jnp.bfloat16)
    ones = jnp.ones((seqs, 128), jnp.bfloat16)
    v_scr[0] = jnp.concatenate([v[:, :128], ones], axis=1)
    v_scr[1] = jnp.concatenate([v[:, 128:], ones], axis=1)
    lane = lax.broadcasted_iota(jnp.int32, (seqs, 256), 1)
    factor = math.log2(math.e) / math.sqrt(HEAD)

    def one_group(group, carry):
        total = None
        for k in range(HEADS // 2):
            q = jnp.where(
                lane // HEAD == group * 4 + k, q_scr[...], jnp.zeros((), jnp.bfloat16)
            )
            scores = mm(q, kt_scr[...])
            top = jnp.max(scores, axis=-1, keepdims=True)
            weights = jnp.exp2((scores - top) * factor).astype(jnp.bfloat16)
            values = jnp.where(
                lane % 128 // HEAD == k, v_scr[group], jnp.zeros((), jnp.bfloat16)
            )
            part = mm(weights, values)
            total = part if total is None else total + part
        acc_scr[group] = total
        return carry

    lax.fori_loop(0, 2, one_group, 0)
    attended = jnp.concatenate(
        [
            acc_scr[0, :, :128] / acc_scr[0, :, 128:],
            acc_scr[1, :, :128] / acc_scr[1, :, 128:],
        ],
        axis=1,
    )
    gate = jax.nn.sigmoid(mm(normed, wg_ref[...]))
    mixed = (attended * gate).astype(jnp.bfloat16)
    first = x + mm(mixed, wo_ref[...])
    hidden = jnp.maximum(
        mm(standardize_features(first).astype(jnp.bfloat16), we_ref[...]), 0.0
    ).astype(jnp.bfloat16)
    second = first + mm(hidden, ws_ref[...])
    out_ref[...] = second.astype(jnp.bfloat16)
    factors = mm(standardize_features(second).astype(jnp.bfloat16), factor_ref[...])
    fac_scr[...] = jnp.where(lane % 128 // HEAD == step, factors, fac_scr[...])

    @pl.when(step == pl.num_programs(0) - 1)
    def _():
        a_ref[:seqs, :] = fac_scr[:, :128].astype(jnp.bfloat16)
        b_ref[:128, :] = fac_scr[:, 128:].T.astype(jnp.bfloat16)
        feat = feat_ref[...]
        a_ref[seqs:, :] = mm(feat, row_ref[...]).astype(jnp.bfloat16)
        b_ref[128:, :128] = mm(feat, column_ref[...]).astype(jnp.bfloat16)
        b_ref[128:, 128:] = jnp.zeros((16, seqs - 128), jnp.bfloat16)


def run_attention(x, feat, weights, interpret=False):
    count_res, seqs, width = x.shape
    whole = [resident(one.shape) for one in (feat,) + weights]
    return pl.pallas_call(
        column_attention,
        grid=(count_res,),
        in_specs=[pl.BlockSpec((1, seqs, width), lambda i: (i, 0, 0))] + whole,
        out_specs=[
            pl.BlockSpec((seqs, width), lambda i: (0, i)),
            FULL,
            FULL,
        ],
        out_shape=[
            jax.ShapeDtypeStruct((seqs, count_res * width), jnp.bfloat16),
            jax.ShapeDtypeStruct((seqs + 16, 128), jnp.bfloat16),
            jax.ShapeDtypeStruct((144, seqs), jnp.bfloat16),
        ],
        scratch_shapes=[
            pltpu.VMEM((seqs, width), jnp.bfloat16),
            pltpu.VMEM((width, seqs), jnp.bfloat16),
            pltpu.VMEM((2, seqs, width), jnp.bfloat16),
            pltpu.VMEM((2, seqs, width), jnp.float32),
            pltpu.VMEM((seqs, width), jnp.float32),
        ],
        compiler_params=pltpu.CompilerParams(
            dimension_semantics=("arbitrary",), vmem_limit_bytes=VMEM_LIMIT
        ),
        name="column_attention",
    )(x, feat, *weights)


def spread_factors(a_ref, b_ref, a_all, b_all, a_send, a_recv, b_send, b_recv):
    rows, cols = lax.axis_size("row"), lax.axis_size("col")
    half = cols // 2
    r, c = lax.axis_index("row"), lax.axis_index("col")
    high, within = c // half, c % half
    core = c % 2
    other_core = c + 1 - 2 * core
    other_high = (1 - high) * half + within
    other_row = r + 1 - 2 * (r % 2)
    ahead = 2 - 4 * core

    def along_x(column, shift):
        return column // half * half + (column % half + shift + half) % half

    def along_y(row, shift):
        return (row + shift + rows) % rows

    spot = within + 1 - 2 * (within % 2)
    first_dest = (spot, 2 * r + high)
    kept = other_row
    first_origin = (c // 2, c % 2 * half + kept)
    barrier = pltpu.get_barrier_semaphore()
    peers = [
        (r, other_core),
        (r, other_high),
        (r, along_x(c, 2)),
        (r, along_x(c, -2)),
        (other_row, c),
        (along_y(r, 2), c),
        (along_y(r, -2), c),
        first_dest,
        first_origin,
    ]
    for peer in peers:
        pl.semaphore_signal(barrier, inc=1, device_id=peer, device_id_type=MESH)
    pl.semaphore_wait(barrier, len(peers))
    sent = []

    def send(src, full, slot, sends, recvs, number, device):
        copy = pltpu.make_async_remote_copy(
            src_ref=src,
            dst_ref=full.at[slot],
            send_sem=sends.at[number],
            recv_sem=recvs.at[slot],
            device_id=device,
            device_id_type=MESH,
        )
        copy.start()
        sent.append(copy)

    def send_a(src, slot, number, column):
        send(src, a_all, slot, a_send, a_recv, number, (r, column))

    def send_b(src, slot, number, device):
        send(src, b_all, slot, b_send, b_recv, number, device)

    def arrived(full, slot, recvs):
        pltpu.make_async_remote_copy(
            src_ref=full.at[slot],
            dst_ref=full.at[slot],
            send_sem=recvs.at[slot],
            recv_sem=recvs.at[slot],
            device_id=(r, other_core),
            device_id_type=MESH,
        ).wait_recv()

    send_b(b_ref, within, 0, first_dest)
    send_a(a_ref, c, 0, other_high)
    send_a(a_ref, c, 1, along_x(c, ahead))
    send_a(a_ref, c, 2, along_x(c, -ahead))
    send_a(a_ref, c, 3, other_core)
    a_all[c] = a_ref[...]
    arrived(b_all, kept, b_recv)
    send_b(b_all.at[kept], kept, 1, (other_row, c))
    send_b(b_all.at[kept], kept, 2, (along_y(r, ahead), c))
    send_b(b_all.at[kept], kept, 3, (along_y(r, -ahead), c))
    arrived(a_all, other_high, a_recv)
    send_a(a_all.at[other_high], other_high, 4, along_x(c, ahead))
    send_a(a_all.at[other_high], other_high, 5, along_x(c, -ahead))
    send_a(a_all.at[other_high], other_high, 6, other_core)
    arrived(b_all, r, b_recv)
    send_b(b_all.at[r], r, 4, (along_y(r, ahead), c))
    send_b(b_all.at[r], r, 5, (along_y(r, -ahead), c))
    for turn, (a_slot, b_slot) in enumerate(((c, kept), (other_high, r))):
        back = along_x(a_slot, -ahead)
        arrived(a_all, back, a_recv)
        send_a(a_all.at[back], back, 7 + 4 * turn, along_x(c, ahead))
        send_a(a_all.at[back], back, 8 + 4 * turn, other_core)
        behind = along_y(b_slot, -ahead)
        arrived(b_all, behind, b_recv)
        send_b(b_all.at[behind], behind, 6 + turn, (along_y(r, ahead), c))
        front = along_x(a_slot, ahead)
        arrived(a_all, front, a_recv)
        send_a(a_all.at[front], front, 9 + 4 * turn, other_core)
    for turn, a_slot in enumerate((c, other_high)):
        far = along_x(a_slot, 4)
        arrived(a_all, far, a_recv)
        send_a(a_all.at[far], far, 10 + 4 * turn, other_core)
    for b_slot in (kept, r):
        arrived(b_all, along_y(b_slot, ahead), b_recv)
        arrived(b_all, along_y(b_slot, 4), b_recv)
    for a_slot in (c, other_high):
        mate = a_slot + 1 - 2 * core
        for shift in range(0, half, 2):
            arrived(a_all, along_x(mate, shift), a_recv)
    for copy in sent:
        copy.wait_send()


def run_spread(a_block, b_block, rows, cols):
    half = cols // 2
    return pl.pallas_call(
        spread_factors,
        in_specs=[FULL, FULL],
        out_specs=[FULL, FULL],
        out_shape=[
            jax.ShapeDtypeStruct((cols,) + a_block.shape, jnp.bfloat16),
            jax.ShapeDtypeStruct((half,) + b_block.shape, jnp.bfloat16),
        ],
        scratch_shapes=[
            pltpu.SemaphoreType.DMA((15,)),
            pltpu.SemaphoreType.DMA((cols,)),
            pltpu.SemaphoreType.DMA((8,)),
            pltpu.SemaphoreType.DMA((half,)),
        ],
        compiler_params=pltpu.CompilerParams(collective_id=0, has_side_effects=True),
        name="spread_factors",
    )(a_block, b_block)


def pair_tile(
    a_ref,
    b_ref,
    offset_ref,
    project_ref,
    expand_ref,
    shrink_ref,
    bins_ref,
    pair_ref,
    distogram_ref,
    c_scr,
    x_scr,
    right_scr,
    own_scr,
    out_scr,
    in_scr,
    turn_scr,
    send_sem,
    recv_sem,
):
    step = pl.program_id(0)
    seqs = b_ref.shape[2]
    r, c = lax.axis_index("row"), lax.axis_index("col")
    mirror_row, parity = c // 2, c % 2
    diagonal = mirror_row == r
    barrier = pltpu.get_barrier_semaphore()

    def mirror_copy(number):
        return pltpu.make_async_remote_copy(
            src_ref=out_scr.at[number],
            dst_ref=in_scr.at[parity, number % 4],
            send_sem=send_sem.at[number],
            recv_sem=recv_sem.at[parity, number % 4],
            device_id=(mirror_row, 2 * r + number // 4),
            device_id_type=MESH,
        )

    def stays(number):
        return jnp.logical_and(diagonal, number // 4 == parity)

    def dispatch(number):
        @pl.when(jnp.logical_not(stays(number)))
        def _():
            mirror_copy(number).start()

    @pl.when(step == 0)
    def _():
        for h in range(2):

            @pl.when(jnp.logical_not(jnp.logical_and(diagonal, parity == h)))
            def _(h=h):
                pl.semaphore_signal(
                    barrier, inc=1, device_id=(mirror_row, 2 * r + h), device_id_type=MESH
                )

    @pl.when(step == 1)
    def _():
        pl.semaphore_wait(barrier, 2 - jnp.where(diagonal, 1, 0))

    @pl.when(step == 0)
    def _():
        for d in range(8):
            right_scr[4 * d : 4 * d + 4, :] = b_ref[d, 128:, :128].astype(jnp.float32)[:4]

    factors = jnp.concatenate([a_ref[2 * step, :seqs, :], a_ref[2 * step + 1, :seqs, :]], axis=1)
    outer = mm(b_ref[:, :128, :].reshape(1024, seqs), factors)
    c_scr[0] = outer[:, :128]
    c_scr[1] = outer[:, 128:]

    @pl.when(step > 0)
    def _():
        dispatch(step - 1)

    lane = lax.broadcasted_iota(jnp.int32, (32, 128), 1)
    low = lane < 64
    even = lane % 64 < 32
    for part in range(2):
        for e in range(0, 32, 4):
            y = [c_scr[part, pl.ds(e + k, 32, stride=32), :] for k in range(4)]
            u = [
                jnp.where(low, y[0], pltpu.roll(y[2], 64, 1)),
                jnp.where(low, y[1], pltpu.roll(y[3], 64, 1)),
                jnp.where(low, pltpu.roll(y[0], 64, 1), y[2]),
                jnp.where(low, pltpu.roll(y[1], 64, 1), y[3]),
            ]
            z = [
                jnp.where(even, u[0], pltpu.roll(u[1], 32, 1)),
                jnp.where(even, pltpu.roll(u[0], 96, 1), u[1]),
                jnp.where(even, u[2], pltpu.roll(u[3], 32, 1)),
                jnp.where(even, pltpu.roll(u[2], 96, 1), u[3]),
            ]
            for i in range(4):
                row = (part * 4 + i) * 32
                x_scr[row : row + 32, e * 32 : e * 32 + 128] = (z[i] * (1.0 / seqs)).astype(
                    jnp.bfloat16
                )
    projected = mm(x_scr[...], project_ref[...])
    index = lax.broadcasted_iota(jnp.int32, (256, 128), 0)
    bins = lax.broadcasted_iota(jnp.int32, (256, 128), 1)
    offset = (c * 32 + index % 32) - (r * 64 + step * 8 + index // 32)
    onehot = jnp.where(jnp.clip(offset, -CLIP, CLIP) + CLIP == bins, 1.0, 0.0)
    relative = mm(onehot.astype(jnp.bfloat16), offset_ref[...])
    left0 = a_ref[2 * step, seqs:, :].astype(jnp.float32)
    left1 = a_ref[2 * step + 1, seqs:, :].astype(jnp.float32)
    left = [left0[i : i + 1] for i in range(4)] + [left1[i : i + 1] for i in range(4)]
    right = right_scr[...]
    embedded = jnp.concatenate([right + one for one in left], axis=0)
    start = embedded + relative + projected
    hidden = jnp.maximum(
        mm(standardize_features(start).astype(jnp.bfloat16), expand_ref[...]), 0.0
    ).astype(jnp.bfloat16)
    final = (start + mm(hidden, shrink_ref[...])).astype(jnp.bfloat16)
    pair_ref[...] = final.reshape(8, 32, 128)
    logits = mm(final, bins_ref[...])
    own_scr[step] = logits
    packed = jnp.where(bins[:128] < 64, logits[:128], logits[128:]).astype(jnp.bfloat16)
    out_scr[step] = packed

    @pl.when(stays(step))
    def _():
        in_scr[parity, step % 4] = packed

    @pl.when(step == pl.num_programs(0) - 1)
    def _():
        dispatch(step)
        for quarter in range(4):
            for k in range(2):

                @pl.when(jnp.logical_not(jnp.logical_and(diagonal, parity == k)))
                def _(k=k, quarter=quarter):
                    pltpu.make_async_remote_copy(
                        src_ref=in_scr.at[k, quarter],
                        dst_ref=in_scr.at[k, quarter],
                        send_sem=recv_sem.at[k, quarter],
                        recv_sem=recv_sem.at[k, quarter],
                        device_id=(mirror_row, 2 * r + k),
                        device_id_type=MESH,
                    ).wait_recv()

                for i in range(4):
                    rows = in_scr[k, quarter, 32 * i : 32 * i + 32, :].astype(jnp.float32)
                    first = k * 1024 + quarter * 8 + i
                    turn_scr[pl.ds(first, 32, stride=32), :] = rows
                    turn_scr[pl.ds(first + 4, 32, stride=32), :] = pltpu.roll(rows, 64, 1)
        for number in range(8):
            total = own_scr[number] + turn_scr[256 * number : 256 * number + 256, :]
            distogram_ref[8 * number : 8 * number + 8] = (
                total[:, :64].astype(jnp.bfloat16).reshape(8, 32, 64)
            )
        for number in range(8):

            @pl.when(jnp.logical_not(stays(number)))
            def _(number=number):
                mirror_copy(number).wait_send()


def run_pair(a_all, b_all, offset, project, expand, shrink, bins):
    return pl.pallas_call(
        pair_tile,
        grid=(8,),
        in_specs=[FULL, FULL]
        + [resident(one.shape) for one in (offset, project, expand, shrink, bins)],
        out_specs=[
            pl.BlockSpec((8, 32, 128), lambda i: (i, 0, 0)),
            pl.BlockSpec((64, 32, 64), lambda i: (0, 0, 0)),
        ],
        out_shape=[
            jax.ShapeDtypeStruct((64, 32, 128), jnp.bfloat16),
            jax.ShapeDtypeStruct((64, 32, 64), jnp.bfloat16),
        ],
        scratch_shapes=[
            pltpu.VMEM((2, 1024, 128), jnp.float32),
            pltpu.VMEM((256, 1024), jnp.bfloat16),
            pltpu.VMEM((32, 128), jnp.float32),
            pltpu.VMEM((8, 256, 128), jnp.float32),
            pltpu.VMEM((8, 128, 128), jnp.bfloat16),
            pltpu.VMEM((2, 4, 128, 128), jnp.bfloat16),
            pltpu.VMEM((2048, 128), jnp.float32),
            pltpu.SemaphoreType.DMA((8,)),
            pltpu.SemaphoreType.DMA((2, 4)),
        ],
        compiler_params=pltpu.CompilerParams(
            dimension_semantics=("arbitrary",),
            vmem_limit_bytes=VMEM_LIMIT,
            collective_id=1,
            has_side_effects=True,
        ),
        name="pair_tile",
    )(a_all, b_all, offset, project, expand, shrink, bins)


def shards(
    homolog_stack,
    per_amino_features,
    asking_matrix,
    lookup_matrix,
    content_matrix,
    sigmoid_scaling_matrix,
    attention_result_matrix,
    stack_transition_expand_matrix,
    stack_transition_shrink_matrix,
    former_factor_matrix,
    latter_factor_matrix,
    factor_mean_projection,
    row_amino_embedding,
    column_amino_embedding,
    offset_embedding_matrix,
    grid_transition_expand,
    grid_transition_shrink,
    distance_bins_matrix,
):
    rows = lax.axis_size("row")
    cols = lax.axis_size("col")
    whole = rows * cols
    seq_here, residues, width = homolog_stack.shape
    res_here = residues // whole
    fragments = homolog_stack.reshape(1, seq_here, whole, res_here, width)
    moved = lax.all_to_all(fragments, ("row", "col"), split_axis=2, concat_axis=0, tiled=True)
    local = moved.reshape(-1, res_here, width)
    seqs = local.shape[0]
    both = jnp.concatenate(
        [jnp.tile(former_factor_matrix, (1, 4)), jnp.tile(latter_factor_matrix, (1, 4))], axis=1
    )
    updated, a_block, b_block = run_attention(
        local.transpose(1, 0, 2),
        jnp.pad(per_amino_features, ((0, 12), (0, 0))),
        (
            asking_matrix,
            lookup_matrix,
            content_matrix,
            sigmoid_scaling_matrix,
            attention_result_matrix,
            stack_transition_expand_matrix,
            stack_transition_shrink_matrix,
            both,
            row_amino_embedding,
            column_amino_embedding,
        ),
    )
    alignment_output = updated.reshape(seqs, res_here, width)
    a_all, b_all = run_spread(a_block, b_block, rows, cols)
    factor = former_factor_matrix.shape[1]
    project = (
        factor_mean_projection.reshape(factor, factor, -1)
        .transpose(1, 0, 2)
        .reshape(factor * factor, -1)
    )
    pair_output, distogram = run_pair(
        a_all,
        b_all,
        jnp.pad(offset_embedding_matrix, ((0, 127 - 2 * CLIP), (0, 0))),
        project,
        grid_transition_expand,
        grid_transition_shrink,
        jnp.concatenate([distance_bins_matrix] * 2, axis=1),
    )
    return (alignment_output, pair_output, distogram)


def solution(mesh):
    placed = (P(("row", "col"), None, None), P(("row", "col"), None)) + (P(),) * 16
    return jax.shard_map(
        shards,
        mesh=mesh,
        in_specs=placed,
        out_specs=(P(None, ("row", "col"), None), P("row", "col", None), P("row", "col", None)),
        check_vma=False,
    )
```

```python
import functools
import math

import jax
import jax.numpy as jnp
from jax import lax
from jax.experimental import pallas as pl
from jax.experimental.pallas import tpu as pltpu
from jax.sharding import PartitionSpec as P

HEADS = 8
HEAD = 32
CLIP = 32
VMEM_LIMIT = 67043328
MESH = pl.DeviceIdType.MESH
FULL = pl.BlockSpec(memory_space=pltpu.VMEM)


def standardize_features(values):
    middle = jnp.mean(values, -1, keepdims=True)
    centred = values - middle
    spread = jnp.mean(centred * centred, -1, keepdims=True)
    return centred * lax.rsqrt(spread + 1e-05)


def resident(shape):
    return pl.BlockSpec(shape, lambda i: (0,) * len(shape))


def mm(a, b):
    return jnp.dot(a, b, preferred_element_type=jnp.float32)


def column_attention(
    x_ref,
    feat_ref,
    wq_ref,
    wk_ref,
    wv_ref,
    wg_ref,
    wo_ref,
    we_ref,
    ws_ref,
    factor_ref,
    row_ref,
    column_ref,
    out_ref,
    a_ref,
    b_ref,
    q_scr,
    kt_scr,
    v_scr,
    acc_scr,
    fac_scr,
):
    step = pl.program_id(0)
    seqs = x_ref.shape[1]
    x = x_ref[0].astype(jnp.float32)
    normed = standardize_features(x).astype(jnp.bfloat16)
    q_scr[...] = mm(normed, wq_ref[...]).astype(jnp.bfloat16)
    kt_scr[...] = mm(normed, wk_ref[...]).T.astype(jnp.bfloat16)
    v = mm(normed, wv_ref[...]).astype(jnp.bfloat16)
    ones = jnp.ones((seqs, 128), jnp.bfloat16)
    v_scr[0] = jnp.concatenate([v[:, :128], ones], axis=1)
    v_scr[1] = jnp.concatenate([v[:, 128:], ones], axis=1)
    lane = lax.broadcasted_iota(jnp.int32, (seqs, 256), 1)
    factor = math.log2(math.e) / math.sqrt(HEAD)

    def one_group(group, carry):
        total = None
        for k in range(HEADS // 2):
            q = jnp.where(
                lane // HEAD == group * 4 + k, q_scr[...], jnp.zeros((), jnp.bfloat16)
            )
            scores = mm(q, kt_scr[...])
            top = jnp.max(scores, axis=-1, keepdims=True)
            weights = jnp.exp2((scores - top) * factor).astype(jnp.bfloat16)
            values = jnp.where(
                lane % 128 // HEAD == k, v_scr[group], jnp.zeros((), jnp.bfloat16)
            )
            part = mm(weights, values)
            total = part if total is None else total + part
        acc_scr[group] = total
        return carry

    lax.fori_loop(0, 2, one_group, 0)
    attended = jnp.concatenate(
        [
            acc_scr[0, :, :128] / acc_scr[0, :, 128:],
            acc_scr[1, :, :128] / acc_scr[1, :, 128:],
        ],
        axis=1,
    )
    gate = jax.nn.sigmoid(mm(normed, wg_ref[...]))
    mixed = (attended * gate).astype(jnp.bfloat16)
    first = x + mm(mixed, wo_ref[...])
    hidden = jnp.maximum(
        mm(standardize_features(first).astype(jnp.bfloat16), we_ref[...]), 0.0
    ).astype(jnp.bfloat16)
    second = first + mm(hidden, ws_ref[...])
    out_ref[...] = second.astype(jnp.bfloat16)
    factors = mm(standardize_features(second).astype(jnp.bfloat16), factor_ref[...])
    fac_scr[...] = jnp.where(lane % 128 // HEAD == step, factors, fac_scr[...])

    @pl.when(step == pl.num_programs(0) - 1)
    def _():
        a_ref[:seqs, :] = fac_scr[:, :128].astype(jnp.bfloat16)
        b_ref[:128, :] = fac_scr[:, 128:].T.astype(jnp.bfloat16)
        feat = feat_ref[...]
        a_ref[seqs:, :] = mm(feat, row_ref[...]).astype(jnp.bfloat16)
        b_ref[128:, :128] = mm(feat, column_ref[...]).astype(jnp.bfloat16)
        b_ref[128:, 128:] = jnp.zeros((16, seqs - 128), jnp.bfloat16)


def run_attention(x, feat, weights, interpret=False):
    count_res, seqs, width = x.shape
    whole = [resident(one.shape) for one in (feat,) + weights]
    return pl.pallas_call(
        column_attention,
        grid=(count_res,),
        in_specs=[pl.BlockSpec((1, seqs, width), lambda i: (i, 0, 0))] + whole,
        out_specs=[
            pl.BlockSpec((seqs, width), lambda i: (0, i)),
            FULL,
            FULL,
        ],
        out_shape=[
            jax.ShapeDtypeStruct((seqs, count_res * width), jnp.bfloat16),
            jax.ShapeDtypeStruct((seqs + 16, 128), jnp.bfloat16),
            jax.ShapeDtypeStruct((144, seqs), jnp.bfloat16),
        ],
        scratch_shapes=[
            pltpu.VMEM((seqs, width), jnp.bfloat16),
            pltpu.VMEM((width, seqs), jnp.bfloat16),
            pltpu.VMEM((2, seqs, width), jnp.bfloat16),
            pltpu.VMEM((2, seqs, width), jnp.float32),
            pltpu.VMEM((seqs, width), jnp.float32),
        ],
        compiler_params=pltpu.CompilerParams(
            dimension_semantics=("arbitrary",), vmem_limit_bytes=VMEM_LIMIT
        ),
        name="column_attention",
    )(x, feat, *weights)


def spread_factors(a_ref, b_ref, a_all, b_all, a_send, a_recv, b_send, b_recv):
    rows, cols = lax.axis_size("row"), lax.axis_size("col")
    half = cols // 2
    r, c = lax.axis_index("row"), lax.axis_index("col")
    high, within = c // half, c % half
    core = c % 2
    other_core = c + 1 - 2 * core
    other_high = (1 - high) * half + within
    other_row = r + 1 - 2 * (r % 2)
    ahead = 2 - 4 * core

    def along_x(column, shift):
        return column // half * half + (column % half + shift + half) % half

    def along_y(row, shift):
        return (row + shift + rows) % rows

    spot = within + 1 - 2 * (within % 2)
    first_dest = (spot, 2 * r + high)
    kept = other_row
    first_origin = (c // 2, c % 2 * half + kept)
    barrier = pltpu.get_barrier_semaphore()
    peers = [
        (r, other_core),
        (r, other_high),
        (r, along_x(c, 2)),
        (r, along_x(c, -2)),
        (other_row, c),
        (along_y(r, 2), c),
        (along_y(r, -2), c),
        first_dest,
        first_origin,
    ]
    for peer in peers:
        pl.semaphore_signal(barrier, inc=1, device_id=peer, device_id_type=MESH)
    pl.semaphore_wait(barrier, len(peers))
    sent = []

    def send(src, full, slot, sends, recvs, number, device):
        copy = pltpu.make_async_remote_copy(
            src_ref=src,
            dst_ref=full.at[slot],
            send_sem=sends.at[number],
            recv_sem=recvs.at[slot],
            device_id=device,
            device_id_type=MESH,
        )
        copy.start()
        sent.append(copy)

    def send_a(src, slot, number, column):
        send(src, a_all, slot, a_send, a_recv, number, (r, column))

    def send_b(src, slot, number, device):
        send(src, b_all, slot, b_send, b_recv, number, device)

    def arrived(full, slot, recvs):
        pltpu.make_async_remote_copy(
            src_ref=full.at[slot],
            dst_ref=full.at[slot],
            send_sem=recvs.at[slot],
            recv_sem=recvs.at[slot],
            device_id=(r, other_core),
            device_id_type=MESH,
        ).wait_recv()

    send_b(b_ref, within, 0, first_dest)
    send_a(a_ref, c, 0, other_high)
    send_a(a_ref, c, 1, along_x(c, ahead))
    send_a(a_ref, c, 2, along_x(c, -ahead))
    send_a(a_ref, c, 3, other_core)
    a_all[c] = a_ref[...]
    arrived(b_all, kept, b_recv)
    send_b(b_all.at[kept], kept, 1, (other_row, c))
    send_b(b_all.at[kept], kept, 2, (along_y(r, ahead), c))
    send_b(b_all.at[kept], kept, 3, (along_y(r, -ahead), c))
    arrived(a_all, other_high, a_recv)
    send_a(a_all.at[other_high], other_high, 4, along_x(c, ahead))
    send_a(a_all.at[other_high], other_high, 5, along_x(c, -ahead))
    send_a(a_all.at[other_high], other_high, 6, other_core)
    arrived(b_all, r, b_recv)
    send_b(b_all.at[r], r, 4, (along_y(r, ahead), c))
    send_b(b_all.at[r], r, 5, (along_y(r, -ahead), c))
    for turn, (a_slot, b_slot) in enumerate(((c, kept), (other_high, r))):
        back = along_x(a_slot, -ahead)
        arrived(a_all, back, a_recv)
        send_a(a_all.at[back], back, 7 + 4 * turn, along_x(c, ahead))
        send_a(a_all.at[back], back, 8 + 4 * turn, other_core)
        behind = along_y(b_slot, -ahead)
        arrived(b_all, behind, b_recv)
        send_b(b_all.at[behind], behind, 6 + turn, (along_y(r, ahead), c))
        front = along_x(a_slot, ahead)
        arrived(a_all, front, a_recv)
        send_a(a_all.at[front], front, 9 + 4 * turn, other_core)
    for turn, a_slot in enumerate((c, other_high)):
        far = along_x(a_slot, 4)
        arrived(a_all, far, a_recv)
        send_a(a_all.at[far], far, 10 + 4 * turn, other_core)
    for b_slot in (kept, r):
        arrived(b_all, along_y(b_slot, ahead), b_recv)
        arrived(b_all, along_y(b_slot, 4), b_recv)
    for a_slot in (c, other_high):
        mate = a_slot + 1 - 2 * core
        for shift in range(0, half, 2):
            arrived(a_all, along_x(mate, shift), a_recv)
    for copy in sent:
        copy.wait_send()


def run_spread(a_block, b_block, rows, cols):
    half = cols // 2
    return pl.pallas_call(
        spread_factors,
        in_specs=[FULL, FULL],
        out_specs=[FULL, FULL],
        out_shape=[
            jax.ShapeDtypeStruct((cols,) + a_block.shape, jnp.bfloat16),
            jax.ShapeDtypeStruct((half,) + b_block.shape, jnp.bfloat16),
        ],
        scratch_shapes=[
            pltpu.SemaphoreType.DMA((15,)),
            pltpu.SemaphoreType.DMA((cols,)),
            pltpu.SemaphoreType.DMA((8,)),
            pltpu.SemaphoreType.DMA((half,)),
        ],
        compiler_params=pltpu.CompilerParams(collective_id=0, has_side_effects=True),
        name="spread_factors",
    )(a_block, b_block)


def pair_tile(
    a_ref,
    b_ref,
    offset_ref,
    project_ref,
    expand_ref,
    shrink_ref,
    bins_ref,
    pair_ref,
    distogram_ref,
    c_scr,
    x_scr,
    right_scr,
    own_scr,
    out_scr,
    in_scr,
    turn_scr,
    send_sem,
    recv_sem,
):
    step = pl.program_id(0)
    seqs = b_ref.shape[2]
    r, c = lax.axis_index("row"), lax.axis_index("col")
    mirror_row, parity = c // 2, c % 2
    diagonal = mirror_row == r
    barrier = pltpu.get_barrier_semaphore()

    def mirror_copy(number):
        return pltpu.make_async_remote_copy(
            src_ref=out_scr.at[number],
            dst_ref=in_scr.at[parity, number % 2],
            send_sem=send_sem.at[number],
            recv_sem=recv_sem.at[parity, number % 2],
            device_id=(mirror_row, 2 * r + number // 2),
            device_id_type=MESH,
        )

    def stays(number):
        return jnp.logical_and(diagonal, number // 2 == parity)

    def dispatch(number):
        @pl.when(jnp.logical_not(stays(number)))
        def _():
            mirror_copy(number).start()

    @pl.when(step == 0)
    def _():
        for h in range(2):

            @pl.when(jnp.logical_not(jnp.logical_and(diagonal, parity == h)))
            def _(h=h):
                pl.semaphore_signal(
                    barrier, inc=1, device_id=(mirror_row, 2 * r + h), device_id_type=MESH
                )

    @pl.when(step == 1)
    def _():
        pl.semaphore_wait(barrier, 2 - jnp.where(diagonal, 1, 0))

    @pl.when(step == 0)
    def _():
        for d in range(8):
            right_scr[4 * d : 4 * d + 4, :] = b_ref[d, 128:, :128].astype(jnp.float32)[:4]

    factors = jnp.concatenate([a_ref[4 * step + n, :seqs, :] for n in range(4)], axis=1)
    outer = mm(b_ref[:, :128, :].reshape(1024, seqs), factors)
    for part in range(4):
        c_scr[part] = outer[:, 128 * part : 128 * part + 128]

    @pl.when(step > 0)
    def _():
        dispatch(step - 1)

    for part in range(4):
        block = (c_scr[part].reshape(32, 32, 128) * (1.0 / seqs)).astype(jnp.bfloat16)
        x_scr[128 * part : 128 * part + 128, :] = jnp.concatenate(
            [block[:, :, 32 * i : 32 * i + 32].reshape(32, 1024) for i in range(4)], axis=0
        )
    projected = mm(x_scr[...], project_ref[...])
    index = lax.broadcasted_iota(jnp.int32, (512, 128), 0)
    bins = lax.broadcasted_iota(jnp.int32, (512, 128), 1)
    offset = (c * 32 + index % 32) - (r * 64 + step * 16 + index // 32)
    onehot = jnp.where(jnp.clip(offset, -CLIP, CLIP) + CLIP == bins, 1.0, 0.0)
    relative = mm(onehot.astype(jnp.bfloat16), offset_ref[...])
    left = []
    for n in range(4):
        four = a_ref[4 * step + n, seqs:, :].astype(jnp.float32)
        left += [four[i : i + 1] for i in range(4)]
    right = right_scr[...]
    embedded = jnp.concatenate([right + one for one in left], axis=0)
    start = embedded + relative + projected
    hidden = jnp.maximum(
        mm(standardize_features(start).astype(jnp.bfloat16), expand_ref[...]), 0.0
    ).astype(jnp.bfloat16)
    final = (start + mm(hidden, shrink_ref[...])).astype(jnp.bfloat16)
    pair_ref[...] = final.reshape(16, 32, 128)
    logits = mm(final, bins_ref[...])
    own_scr[step] = logits
    packed = jnp.where(bins[:256] < 64, logits[:256], logits[256:]).astype(jnp.bfloat16)
    out_scr[step] = packed

    @pl.when(stays(step))
    def _():
        in_scr[parity, step % 2] = packed

    @pl.when(step == pl.num_programs(0) - 1)
    def _():
        dispatch(step)
        for quarter in range(2):
            for k in range(2):

                @pl.when(jnp.logical_not(jnp.logical_and(diagonal, parity == k)))
                def _(k=k, quarter=quarter):
                    pltpu.make_async_remote_copy(
                        src_ref=in_scr.at[k, quarter],
                        dst_ref=in_scr.at[k, quarter],
                        send_sem=recv_sem.at[k, quarter],
                        recv_sem=recv_sem.at[k, quarter],
                        device_id=(mirror_row, 2 * r + k),
                        device_id_type=MESH,
                    ).wait_recv()

                for i in range(8):
                    rows = in_scr[k, quarter, 32 * i : 32 * i + 32, :].astype(jnp.float32)
                    first = k * 1024 + quarter * 16 + i
                    turn_scr[pl.ds(first, 32, stride=32), :] = rows
                    turn_scr[pl.ds(first + 8, 32, stride=32), :] = pltpu.roll(rows, 64, 1)
        for number in range(4):
            total = own_scr[number] + turn_scr[512 * number : 512 * number + 512, :]
            distogram_ref[16 * number : 16 * number + 16] = (
                total[:, :64].astype(jnp.bfloat16).reshape(16, 32, 64)
            )
        for number in range(4):

            @pl.when(jnp.logical_not(stays(number)))
            def _(number=number):
                mirror_copy(number).wait_send()


def run_pair(a_all, b_all, offset, project, expand, shrink, bins):
    return pl.pallas_call(
        pair_tile,
        grid=(4,),
        in_specs=[FULL, FULL]
        + [resident(one.shape) for one in (offset, project, expand, shrink, bins)],
        out_specs=[
            pl.BlockSpec((16, 32, 128), lambda i: (i, 0, 0)),
            pl.BlockSpec((64, 32, 64), lambda i: (0, 0, 0)),
        ],
        out_shape=[
            jax.ShapeDtypeStruct((64, 32, 128), jnp.bfloat16),
            jax.ShapeDtypeStruct((64, 32, 64), jnp.bfloat16),
        ],
        scratch_shapes=[
            pltpu.VMEM((4, 1024, 128), jnp.float32),
            pltpu.VMEM((512, 1024), jnp.bfloat16),
            pltpu.VMEM((32, 128), jnp.float32),
            pltpu.VMEM((4, 512, 128), jnp.float32),
            pltpu.VMEM((4, 256, 128), jnp.bfloat16),
            pltpu.VMEM((2, 2, 256, 128), jnp.bfloat16),
            pltpu.VMEM((2048, 128), jnp.float32),
            pltpu.SemaphoreType.DMA((4,)),
            pltpu.SemaphoreType.DMA((2, 2)),
        ],
        compiler_params=pltpu.CompilerParams(
            dimension_semantics=("arbitrary",),
            vmem_limit_bytes=VMEM_LIMIT,
            collective_id=1,
            has_side_effects=True,
        ),
        name="pair_tile",
    )(a_all, b_all, offset, project, expand, shrink, bins)


def shards(
    homolog_stack,
    per_amino_features,
    asking_matrix,
    lookup_matrix,
    content_matrix,
    sigmoid_scaling_matrix,
    attention_result_matrix,
    stack_transition_expand_matrix,
    stack_transition_shrink_matrix,
    former_factor_matrix,
    latter_factor_matrix,
    factor_mean_projection,
    row_amino_embedding,
    column_amino_embedding,
    offset_embedding_matrix,
    grid_transition_expand,
    grid_transition_shrink,
    distance_bins_matrix,
):
    rows = lax.axis_size("row")
    cols = lax.axis_size("col")
    whole = rows * cols
    seq_here, residues, width = homolog_stack.shape
    res_here = residues // whole
    fragments = homolog_stack.reshape(1, seq_here, whole, res_here, width)
    moved = lax.all_to_all(fragments, ("row", "col"), split_axis=2, concat_axis=0, tiled=True)
    local = moved.reshape(-1, res_here, width)
    seqs = local.shape[0]
    both = jnp.concatenate(
        [jnp.tile(former_factor_matrix, (1, 4)), jnp.tile(latter_factor_matrix, (1, 4))], axis=1
    )
    updated, a_block, b_block = run_attention(
        local.transpose(1, 0, 2),
        jnp.pad(per_amino_features, ((0, 12), (0, 0))),
        (
            asking_matrix,
            lookup_matrix,
            content_matrix,
            sigmoid_scaling_matrix,
            attention_result_matrix,
            stack_transition_expand_matrix,
            stack_transition_shrink_matrix,
            both,
            row_amino_embedding,
            column_amino_embedding,
        ),
    )
    alignment_output = updated.reshape(seqs, res_here, width)
    a_all, b_all = run_spread(a_block, b_block, rows, cols)
    factor = former_factor_matrix.shape[1]
    project = (
        factor_mean_projection.reshape(factor, factor, -1)
        .transpose(1, 0, 2)
        .reshape(factor * factor, -1)
    )
    pair_output, distogram = run_pair(
        a_all,
        b_all,
        jnp.pad(offset_embedding_matrix, ((0, 127 - 2 * CLIP), (0, 0))),
        project,
        grid_transition_expand,
        grid_transition_shrink,
        jnp.concatenate([distance_bins_matrix] * 2, axis=1),
    )
    return (alignment_output, pair_output, distogram)


def solution(mesh):
    placed = (P(("row", "col"), None, None), P(("row", "col"), None)) + (P(),) * 16
    return jax.shard_map(
        shards,
        mesh=mesh,
        in_specs=placed,
        out_specs=(P(None, ("row", "col"), None), P("row", "col", None), P("row", "col", None)),
        check_vma=False,
    )
```

```python
import functools
import math

import jax
import jax.numpy as jnp
from jax import lax
from jax.experimental import pallas as pl
from jax.experimental.pallas import tpu as pltpu
from jax.sharding import PartitionSpec as P

HEADS = 8
HEAD = 32
CLIP = 32
VMEM_LIMIT = 67043328
MESH = pl.DeviceIdType.MESH
FULL = pl.BlockSpec(memory_space=pltpu.VMEM)


def standardize_features(values):
    middle = jnp.mean(values, -1, keepdims=True)
    centred = values - middle
    spread = jnp.mean(centred * centred, -1, keepdims=True)
    return centred * lax.rsqrt(spread + 1e-05)


def resident(shape):
    return pl.BlockSpec(shape, lambda i: (0,) * len(shape))


def mm(a, b):
    return jnp.dot(a, b, preferred_element_type=jnp.float32)


class Spread:
    def __init__(self, own, a_all, b_all, a_send, a_recv, b_send, b_recv):
        self.own, self.a_all, self.b_all = own, a_all, b_all
        self.a_send, self.a_recv, self.b_send, self.b_recv = a_send, a_recv, b_send, b_recv
        self.rows, cols = lax.axis_size("row"), lax.axis_size("col")
        self.half = cols // 2
        r, c = lax.axis_index("row"), lax.axis_index("col")
        high, within = c // self.half, c % self.half
        self.r, self.c, self.within = r, c, within
        self.turned = 1 - 2 * (c % 2)
        self.mate = c + self.turned
        self.other_high = (1 - high) * self.half + within
        self.other_row = r + 1 - 2 * (r % 2)
        self.ahead = 2 * self.turned
        self.first_dest = (within + 1 - 2 * (within % 2), 2 * r + high)
        self.first_origin = (c // 2, c % 2 * self.half + self.other_row)

    def along_x(self, column, shift):
        half = self.half
        return column // half * half + (column % half + shift + half) % half

    def along_y(self, row, shift):
        return (row + shift + self.rows) % self.rows

    def greet(self):
        barrier = pltpu.get_barrier_semaphore()
        r, c = self.r, self.c
        peers = [
            (r, self.mate),
            (r, self.other_high),
            (r, self.along_x(c, 2)),
            (r, self.along_x(c, -2)),
            (self.other_row, c),
            (self.along_y(r, 2), c),
            (self.along_y(r, -2), c),
            self.first_dest,
            self.first_origin,
        ]
        for peer in peers:
            pl.semaphore_signal(barrier, inc=1, device_id=peer, device_id_type=MESH)
        pl.semaphore_wait(barrier, len(peers))

    def copy_a(self, part, slot, number, column):
        return pltpu.make_async_remote_copy(
            src_ref=self.a_all.at[slot, part],
            dst_ref=self.a_all.at[slot, part],
            send_sem=self.a_send.at[part, number],
            recv_sem=self.a_recv.at[part, slot],
            device_id=(self.r, column),
            device_id_type=MESH,
        )

    def copy_b(self, part, slot, number, device, src=None):
        return pltpu.make_async_remote_copy(
            src_ref=self.b_all.at[slot, part] if src is None else src,
            dst_ref=self.b_all.at[slot, part],
            send_sem=self.b_send.at[part, number],
            recv_sem=self.b_recv.at[part, slot],
            device_id=device,
            device_id_type=MESH,
        )

    def wait_a(self, part, slot):
        self.copy_a(part, slot, 0, self.mate).wait_recv()

    def wait_b(self, part, slot):
        self.copy_b(part, slot, 0, (self.other_row, self.c)).wait_recv()

    def begin(self, part):
        c, ahead = self.c, self.ahead
        self.copy_b(part, self.within, 0, self.first_dest, self.own.at[part]).start()
        self.copy_a(part, c, 0, self.other_high).start()
        self.copy_a(part, c, 1, self.along_x(c, ahead)).start()
        self.copy_a(part, c, 2, self.along_x(c, -ahead)).start()
        self.copy_a(part, c, 3, self.mate).start()

    def second(self, part):
        r, c, ahead, kept = self.r, self.c, self.ahead, self.other_row
        self.wait_b(part, kept)
        self.copy_b(part, kept, 1, (self.other_row, c)).start()
        self.copy_b(part, kept, 2, (self.along_y(r, ahead), c)).start()
        self.copy_b(part, kept, 3, (self.along_y(r, -ahead), c)).start()
        self.wait_a(part, self.other_high)
        self.copy_a(part, self.other_high, 4, self.along_x(c, ahead)).start()
        self.copy_a(part, self.other_high, 5, self.along_x(c, -ahead)).start()
        self.copy_a(part, self.other_high, 6, self.mate).start()

    def third(self, part):
        r, c, ahead = self.r, self.c, self.ahead
        self.wait_b(part, r)
        self.copy_b(part, r, 4, (self.along_y(r, ahead), c)).start()
        self.copy_b(part, r, 5, (self.along_y(r, -ahead), c)).start()
        self.relay(part, 0, c, self.other_row)

    def fourth(self, part):
        self.relay(part, 1, self.other_high, self.r)

    def relay(self, part, turn, a_slot, b_slot):
        r, c, ahead = self.r, self.c, self.ahead
        back = self.along_x(a_slot, -ahead)
        self.wait_a(part, back)
        self.copy_a(part, back, 7 + 4 * turn, self.along_x(c, ahead)).start()
        self.copy_a(part, back, 8 + 4 * turn, self.mate).start()
        behind = self.along_y(b_slot, -ahead)
        self.wait_b(part, behind)
        self.copy_b(part, behind, 6 + turn, (self.along_y(r, ahead), c)).start()
        front = self.along_x(a_slot, ahead)
        self.wait_a(part, front)
        self.copy_a(part, front, 9 + 4 * turn, self.mate).start()

    def fifth(self, part):
        for turn, a_slot in enumerate((self.c, self.other_high)):
            far = self.along_x(a_slot, 4)
            self.wait_a(part, far)
            self.copy_a(part, far, 10 + 4 * turn, self.mate).start()

    def finish(self, part):
        for b_slot in (self.other_row, self.r):
            self.wait_b(part, self.along_y(b_slot, self.ahead))
            self.wait_b(part, self.along_y(b_slot, 4))
        for a_slot in (self.c, self.other_high):
            for shift in range(0, self.half, 2):
                self.wait_a(part, self.along_x(a_slot + self.turned, shift))
        for number in range(15):
            self.copy_a(part, self.c, number, self.mate).wait_send()
        for number in range(8):
            self.copy_b(part, self.r, number, (self.other_row, self.c)).wait_send()


def column_attention(
    x_ref,
    feat_ref,
    wq_ref,
    wk_ref,
    wv_ref,
    wg_ref,
    wo_ref,
    we_ref,
    ws_ref,
    factor_ref,
    row_ref,
    column_ref,
    out_ref,
    a_out,
    b_out,
    q_scr,
    kt_scr,
    v_scr,
    acc_scr,
    own_scr,
    a_all,
    b_all,
    a_send,
    a_recv,
    b_send,
    b_recv,
    out_sem,
):
    step = pl.program_id(0)
    seqs = x_ref.shape[1]
    spread = Spread(own_scr, a_all, b_all, a_send, a_recv, b_send, b_recv)

    @pl.when(step == 0)
    def _():
        feat = feat_ref[...]
        a_all[spread.c, 0] = jnp.zeros((32, seqs), jnp.bfloat16)
        own_scr[0] = jnp.zeros((32, seqs), jnp.bfloat16)
        a_all[spread.c, 0, :16, :128] = mm(feat, row_ref[...]).astype(jnp.bfloat16)
        own_scr[0, :16, :128] = mm(feat, column_ref[...]).astype(jnp.bfloat16)
        spread.greet()

    spread.begin(step)
    x = x_ref[0].astype(jnp.float32)
    normed = standardize_features(x).astype(jnp.bfloat16)
    q_scr[...] = mm(normed, wq_ref[...]).astype(jnp.bfloat16)
    kt_scr[...] = mm(normed, wk_ref[...]).T.astype(jnp.bfloat16)
    v = mm(normed, wv_ref[...]).astype(jnp.bfloat16)
    ones = jnp.ones((seqs, 128), jnp.bfloat16)
    v_scr[0] = jnp.concatenate([v[:, :128], ones], axis=1)
    v_scr[1] = jnp.concatenate([v[:, 128:], ones], axis=1)
    lane = lax.broadcasted_iota(jnp.int32, (seqs, 256), 1)
    factor = math.log2(math.e) / math.sqrt(HEAD)

    for group in range(2):
        total = None
        for k in range(HEADS // 2):
            q = jnp.where(
                lane // HEAD == group * 4 + k, q_scr[...], jnp.zeros((), jnp.bfloat16)
            )
            scores = mm(q, kt_scr[...])
            top = jnp.max(scores, axis=-1, keepdims=True)
            weights = jnp.exp2((scores - top) * factor).astype(jnp.bfloat16)
            values = jnp.where(
                lane % 128 // HEAD == k, v_scr[group], jnp.zeros((), jnp.bfloat16)
            )
            part = mm(weights, values)
            total = part if total is None else total + part
        acc_scr[group] = total
    attended = jnp.concatenate(
        [
            acc_scr[0, :, :128] / acc_scr[0, :, 128:],
            acc_scr[1, :, :128] / acc_scr[1, :, 128:],
        ],
        axis=1,
    )
    gate = jax.nn.sigmoid(mm(normed, wg_ref[...]))
    mixed = (attended * gate).astype(jnp.bfloat16)
    first = x + mm(mixed, wo_ref[...])
    hidden = jnp.maximum(
        mm(standardize_features(first).astype(jnp.bfloat16), we_ref[...]), 0.0
    ).astype(jnp.bfloat16)
    second = first + mm(hidden, ws_ref[...])
    out_ref[...] = second.astype(jnp.bfloat16)
    factors = mm(standardize_features(second).astype(jnp.bfloat16), factor_ref[...])
    turned = factors.T.astype(jnp.bfloat16)
    a_all[spread.c, step + 1] = turned[:32]
    own_scr[step + 1] = turned[32:64]
    spread.second(step)

    @pl.when(step > 0)
    def _():
        spread.third(step - 1)

    @pl.when(step > 1)
    def _():
        spread.fourth(step - 2)

    @pl.when(step > 2)
    def _():
        spread.fifth(step - 3)

    last = pl.num_programs(0)

    @pl.when(step == last - 1)
    def _():
        spread.begin(last)
        spread.third(last - 1)
        spread.fourth(last - 2)
        spread.fifth(last - 3)
        spread.second(last)
        spread.fourth(last - 1)
        spread.fifth(last - 2)
        spread.third(last)
        spread.fifth(last - 1)
        spread.fourth(last)
        spread.fifth(last)
        for part in range(5):
            spread.finish(part)
        results = [
            pltpu.make_async_copy(a_all, a_out, out_sem.at[0]),
            pltpu.make_async_copy(b_all, b_out, out_sem.at[1]),
        ]
        for copy in results:
            copy.start()
        for copy in results:
            copy.wait()


def run_attention(x, feat, weights, interpret=False):
    count_res, seqs, width = x.shape
    whole = [resident(one.shape) for one in (feat,) + weights]
    return pl.pallas_call(
        column_attention,
        grid=(count_res,),
        in_specs=[pl.BlockSpec((1, seqs, width), lambda i: (i, 0, 0))] + whole,
        out_specs=[
            pl.BlockSpec((seqs, width), lambda i: (0, i)),
            pl.BlockSpec(memory_space=pl.ANY),
            pl.BlockSpec(memory_space=pl.ANY),
        ],
        out_shape=[
            jax.ShapeDtypeStruct((seqs, count_res * width), jnp.bfloat16),
            jax.ShapeDtypeStruct((16, count_res + 1, 32, seqs), jnp.bfloat16),
            jax.ShapeDtypeStruct((8, count_res + 1, 32, seqs), jnp.bfloat16),
        ],
        scratch_shapes=[
            pltpu.VMEM((seqs, width), jnp.bfloat16),
            pltpu.VMEM((width, seqs), jnp.bfloat16),
            pltpu.VMEM((2, seqs, width), jnp.bfloat16),
            pltpu.VMEM((2, seqs, width), jnp.float32),
            pltpu.VMEM((count_res + 1, 32, seqs), jnp.bfloat16),
            pltpu.VMEM((16, count_res + 1, 32, seqs), jnp.bfloat16),
            pltpu.VMEM((8, count_res + 1, 32, seqs), jnp.bfloat16),
            pltpu.SemaphoreType.DMA((count_res + 1, 15)),
            pltpu.SemaphoreType.DMA((count_res + 1, 16)),
            pltpu.SemaphoreType.DMA((count_res + 1, 8)),
            pltpu.SemaphoreType.DMA((count_res + 1, 8)),
            pltpu.SemaphoreType.DMA((2,)),
        ],
        compiler_params=pltpu.CompilerParams(
            dimension_semantics=("arbitrary",),
            vmem_limit_bytes=VMEM_LIMIT,
            collective_id=0,
            has_side_effects=True,
        ),
        name="column_attention",
    )(x, feat, *weights)


def pair_tile(
    a_ref,
    b_ref,
    offset_ref,
    project_ref,
    expand_ref,
    shrink_ref,
    bins_ref,
    pair_ref,
    distogram_ref,
    c_scr,
    x_scr,
    right_scr,
    own_scr,
    out_scr,
    in_scr,
    turn_scr,
    send_sem,
    recv_sem,
):
    step = pl.program_id(0)
    seqs = b_ref.shape[3]
    r, c = lax.axis_index("row"), lax.axis_index("col")
    mirror_row, parity = c // 2, c % 2
    diagonal = mirror_row == r
    barrier = pltpu.get_barrier_semaphore()

    def mirror_copy(number):
        return pltpu.make_async_remote_copy(
            src_ref=out_scr.at[number],
            dst_ref=in_scr.at[parity, number % 2],
            send_sem=send_sem.at[number],
            recv_sem=recv_sem.at[parity, number % 2],
            device_id=(mirror_row, 2 * r + number // 2),
            device_id_type=MESH,
        )

    def stays(number):
        return jnp.logical_and(diagonal, number // 2 == parity)

    def dispatch(number):
        @pl.when(jnp.logical_not(stays(number)))
        def _():
            mirror_copy(number).start()

    @pl.when(step == 0)
    def _():
        for h in range(2):

            @pl.when(jnp.logical_not(jnp.logical_and(diagonal, parity == h)))
            def _(h=h):
                pl.semaphore_signal(
                    barrier, inc=1, device_id=(mirror_row, 2 * r + h), device_id_type=MESH
                )

    @pl.when(step == 1)
    def _():
        pl.semaphore_wait(barrier, 2 - jnp.where(diagonal, 1, 0))

    @pl.when(step == 0)
    def _():
        for d in range(8):
            right_scr[4 * d : 4 * d + 4, :] = b_ref[d, 0, :16, :128].astype(jnp.float32)[:4]

    factors = a_ref[pl.ds(4 * step, 4), 1:].reshape(512, seqs)
    outer = lax.dot_general(
        b_ref[:, 1:].reshape(1024, seqs),
        factors,
        (((1,), (1,)), ((), ())),
        preferred_element_type=jnp.float32,
    )
    for part in range(4):
        c_scr[part] = outer[:, 128 * part : 128 * part + 128]

    @pl.when(step > 0)
    def _():
        dispatch(step - 1)

    for part in range(4):
        block = (c_scr[part].reshape(32, 32, 128) * (1.0 / seqs)).astype(jnp.bfloat16)
        x_scr[128 * part : 128 * part + 128, :] = jnp.concatenate(
            [block[:, :, 32 * i : 32 * i + 32].reshape(32, 1024) for i in range(4)], axis=0
        )
    projected = mm(x_scr[...], project_ref[...])
    index = lax.broadcasted_iota(jnp.int32, (512, 128), 0)
    bins = lax.broadcasted_iota(jnp.int32, (512, 128), 1)
    offset = (c * 32 + index % 32) - (r * 64 + step * 16 + index // 32)
    onehot = jnp.where(jnp.clip(offset, -CLIP, CLIP) + CLIP == bins, 1.0, 0.0)
    relative = mm(onehot.astype(jnp.bfloat16), offset_ref[...])
    left = []
    for n in range(4):
        four = a_ref[4 * step + n, 0, :16, :128].astype(jnp.float32)
        left += [four[i : i + 1] for i in range(4)]
    right = right_scr[...]
    embedded = jnp.concatenate([right + one for one in left], axis=0)
    start = embedded + relative + projected
    hidden = jnp.maximum(
        mm(standardize_features(start).astype(jnp.bfloat16), expand_ref[...]), 0.0
    ).astype(jnp.bfloat16)
    final = (start + mm(hidden, shrink_ref[...])).astype(jnp.bfloat16)
    pair_ref[...] = final.reshape(16, 32, 128)
    logits = mm(final, bins_ref[...])
    own_scr[step] = logits
    packed = jnp.where(bins[:256] < 64, logits[:256], logits[256:]).astype(jnp.bfloat16)
    out_scr[step] = packed

    @pl.when(stays(step))
    def _():
        in_scr[parity, step % 2] = packed

    @pl.when(step == pl.num_programs(0) - 1)
    def _():
        dispatch(step)
        for quarter in range(2):
            for k in range(2):

                @pl.when(jnp.logical_not(jnp.logical_and(diagonal, parity == k)))
                def _(k=k, quarter=quarter):
                    pltpu.make_async_remote_copy(
                        src_ref=in_scr.at[k, quarter],
                        dst_ref=in_scr.at[k, quarter],
                        send_sem=recv_sem.at[k, quarter],
                        recv_sem=recv_sem.at[k, quarter],
                        device_id=(mirror_row, 2 * r + k),
                        device_id_type=MESH,
                    ).wait_recv()

                for i in range(8):
                    rows = in_scr[k, quarter, 32 * i : 32 * i + 32, :].astype(jnp.float32)
                    first = k * 1024 + quarter * 16 + i
                    turn_scr[pl.ds(first, 32, stride=32), :] = rows
                    turn_scr[pl.ds(first + 8, 32, stride=32), :] = pltpu.roll(rows, 64, 1)
        for number in range(4):
            total = own_scr[number] + turn_scr[512 * number : 512 * number + 512, :]
            distogram_ref[16 * number : 16 * number + 16] = (
                total[:, :64].astype(jnp.bfloat16).reshape(16, 32, 64)
            )
        for number in range(4):

            @pl.when(jnp.logical_not(stays(number)))
            def _(number=number):
                mirror_copy(number).wait_send()


def run_pair(a_all, b_all, offset, project, expand, shrink, bins):
    return pl.pallas_call(
        pair_tile,
        grid=(4,),
        in_specs=[FULL, FULL]
        + [resident(one.shape) for one in (offset, project, expand, shrink, bins)],
        out_specs=[
            pl.BlockSpec((16, 32, 128), lambda i: (i, 0, 0)),
            pl.BlockSpec((64, 32, 64), lambda i: (0, 0, 0)),
        ],
        out_shape=[
            jax.ShapeDtypeStruct((64, 32, 128), jnp.bfloat16),
            jax.ShapeDtypeStruct((64, 32, 64), jnp.bfloat16),
        ],
        scratch_shapes=[
            pltpu.VMEM((4, 1024, 128), jnp.float32),
            pltpu.VMEM((512, 1024), jnp.bfloat16),
            pltpu.VMEM((32, 128), jnp.float32),
            pltpu.VMEM((4, 512, 128), jnp.float32),
            pltpu.VMEM((4, 256, 128), jnp.bfloat16),
            pltpu.VMEM((2, 2, 256, 128), jnp.bfloat16),
            pltpu.VMEM((2048, 128), jnp.float32),
            pltpu.SemaphoreType.DMA((4,)),
            pltpu.SemaphoreType.DMA((2, 2)),
        ],
        compiler_params=pltpu.CompilerParams(
            dimension_semantics=("arbitrary",),
            vmem_limit_bytes=VMEM_LIMIT,
            collective_id=1,
            has_side_effects=True,
        ),
        name="pair_tile",
    )(a_all, b_all, offset, project, expand, shrink, bins)


def shards(
    homolog_stack,
    per_amino_features,
    asking_matrix,
    lookup_matrix,
    content_matrix,
    sigmoid_scaling_matrix,
    attention_result_matrix,
    stack_transition_expand_matrix,
    stack_transition_shrink_matrix,
    former_factor_matrix,
    latter_factor_matrix,
    factor_mean_projection,
    row_amino_embedding,
    column_amino_embedding,
    offset_embedding_matrix,
    grid_transition_expand,
    grid_transition_shrink,
    distance_bins_matrix,
):
    rows = lax.axis_size("row")
    cols = lax.axis_size("col")
    whole = rows * cols
    seq_here, residues, width = homolog_stack.shape
    res_here = residues // whole
    fragments = homolog_stack.reshape(1, seq_here, whole, res_here, width)
    moved = lax.all_to_all(fragments, ("row", "col"), split_axis=2, concat_axis=0, tiled=True)
    local = moved.reshape(-1, res_here, width)
    seqs = local.shape[0]
    both = jnp.concatenate(
        [former_factor_matrix, latter_factor_matrix, jnp.zeros((width, 64), jnp.bfloat16)], axis=1
    )
    updated, a_all, b_all = run_attention(
        local.transpose(1, 0, 2),
        jnp.pad(per_amino_features, ((0, 12), (0, 0))),
        (
            asking_matrix,
            lookup_matrix,
            content_matrix,
            sigmoid_scaling_matrix,
            attention_result_matrix,
            stack_transition_expand_matrix,
            stack_transition_shrink_matrix,
            both,
            row_amino_embedding,
            column_amino_embedding,
        ),
    )
    alignment_output = updated.reshape(seqs, res_here, width)
    factor = former_factor_matrix.shape[1]
    project = (
        factor_mean_projection.reshape(factor, factor, -1)
        .transpose(1, 0, 2)
        .reshape(factor * factor, -1)
    )
    pair_output, distogram = run_pair(
        a_all,
        b_all,
        jnp.pad(offset_embedding_matrix, ((0, 127 - 2 * CLIP), (0, 0))),
        project,
        grid_transition_expand,
        grid_transition_shrink,
        jnp.concatenate([distance_bins_matrix] * 2, axis=1),
    )
    return (alignment_output, pair_output, distogram)


def solution(mesh):
    placed = (P(("row", "col"), None, None), P(("row", "col"), None)) + (P(),) * 16
    return jax.shard_map(
        shards,
        mesh=mesh,
        in_specs=placed,
        out_specs=(P(None, ("row", "col"), None), P("row", "col", None), P("row", "col", None)),
        check_vma=False,
    )
```

```python
import functools
import math

import jax
import jax.numpy as jnp
from jax import lax
from jax.experimental import pallas as pl
from jax.experimental.pallas import tpu as pltpu
from jax.sharding import PartitionSpec as P

HEADS = 8
HEAD = 32
CLIP = 32
VMEM_LIMIT = 67043328
MESH = pl.DeviceIdType.MESH
FULL = pl.BlockSpec(memory_space=pltpu.VMEM)


def standardize_features(values):
    middle = jnp.mean(values, -1, keepdims=True)
    centred = values - middle
    spread = jnp.mean(centred * centred, -1, keepdims=True)
    return centred * lax.rsqrt(spread + 1e-05)


def resident(shape):
    return pl.BlockSpec(shape, lambda i: (0,) * len(shape))


def mm(a, b):
    return jnp.dot(a, b, preferred_element_type=jnp.float32)


class Spread:
    def __init__(self, own, a_all, b_all, a_send, a_recv, b_send, b_recv):
        self.own, self.a_all, self.b_all = own, a_all, b_all
        self.a_send, self.a_recv, self.b_send, self.b_recv = a_send, a_recv, b_send, b_recv
        self.rows, cols = lax.axis_size("row"), lax.axis_size("col")
        self.half = cols // 2
        r, c = lax.axis_index("row"), lax.axis_index("col")
        high, within = c // self.half, c % self.half
        self.r, self.c, self.within = r, c, within
        self.turned = 1 - 2 * (c % 2)
        self.mate = c + self.turned
        self.other_high = (1 - high) * self.half + within
        self.other_row = r + 1 - 2 * (r % 2)
        self.ahead = 2 * self.turned
        self.first_dest = (within + 1 - 2 * (within % 2), 2 * r + high)
        self.first_origin = (c // 2, c % 2 * self.half + self.other_row)

    def along_x(self, column, shift):
        half = self.half
        return column // half * half + (column % half + shift + half) % half

    def along_y(self, row, shift):
        return (row + shift + self.rows) % self.rows

    def greet(self):
        barrier = pltpu.get_barrier_semaphore()
        r, c = self.r, self.c
        peers = [
            (r, self.mate),
            (r, self.other_high),
            (r, self.along_x(c, 2)),
            (r, self.along_x(c, -2)),
            (self.other_row, c),
            (self.along_y(r, 2), c),
            (self.along_y(r, -2), c),
            self.first_dest,
            self.first_origin,
        ]
        for peer in peers:
            pl.semaphore_signal(barrier, inc=1, device_id=peer, device_id_type=MESH)
        pl.semaphore_wait(barrier, len(peers))

    def copy_a(self, part, slot, number, column):
        return pltpu.make_async_remote_copy(
            src_ref=self.a_all.at[slot, part],
            dst_ref=self.a_all.at[slot, part],
            send_sem=self.a_send.at[part, number],
            recv_sem=self.a_recv.at[part, slot],
            device_id=(self.r, column),
            device_id_type=MESH,
        )

    def copy_b(self, part, slot, number, device, src=None):
        return pltpu.make_async_remote_copy(
            src_ref=self.b_all.at[slot, part] if src is None else src,
            dst_ref=self.b_all.at[slot, part],
            send_sem=self.b_send.at[part, number],
            recv_sem=self.b_recv.at[part, slot],
            device_id=device,
            device_id_type=MESH,
        )

    def wait_a(self, part, slot):
        self.copy_a(part, slot, 0, self.mate).wait_recv()

    def wait_b(self, part, slot):
        self.copy_b(part, slot, 0, (self.other_row, self.c)).wait_recv()

    def begin(self, part):
        c, ahead = self.c, self.ahead
        self.copy_b(part, self.within, 0, self.first_dest, self.own.at[part]).start()
        self.copy_a(part, c, 0, self.other_high).start()
        self.copy_a(part, c, 1, self.along_x(c, ahead)).start()
        self.copy_a(part, c, 2, self.along_x(c, -ahead)).start()
        self.copy_a(part, c, 3, self.mate).start()

    def second(self, part):
        r, c, ahead, kept = self.r, self.c, self.ahead, self.other_row
        self.wait_b(part, kept)
        self.copy_b(part, kept, 1, (self.other_row, c)).start()
        self.copy_b(part, kept, 2, (self.along_y(r, ahead), c)).start()
        self.copy_b(part, kept, 3, (self.along_y(r, -ahead), c)).start()
        self.wait_a(part, self.other_high)
        self.copy_a(part, self.other_high, 4, self.along_x(c, ahead)).start()
        self.copy_a(part, self.other_high, 5, self.along_x(c, -ahead)).start()
        self.copy_a(part, self.other_high, 6, self.mate).start()

    def third(self, part):
        r, c, ahead = self.r, self.c, self.ahead
        self.wait_b(part, r)
        self.copy_b(part, r, 4, (self.along_y(r, ahead), c)).start()
        self.copy_b(part, r, 5, (self.along_y(r, -ahead), c)).start()
        self.relay(part, 0, c, self.other_row)

    def fourth(self, part):
        self.relay(part, 1, self.other_high, self.r)

    def relay(self, part, turn, a_slot, b_slot):
        r, c, ahead = self.r, self.c, self.ahead
        back = self.along_x(a_slot, -ahead)
        self.wait_a(part, back)
        self.copy_a(part, back, 7 + 4 * turn, self.along_x(c, ahead)).start()
        self.copy_a(part, back, 8 + 4 * turn, self.mate).start()
        behind = self.along_y(b_slot, -ahead)
        self.wait_b(part, behind)
        self.copy_b(part, behind, 6 + turn, (self.along_y(r, ahead), c)).start()
        front = self.along_x(a_slot, ahead)
        self.wait_a(part, front)
        self.copy_a(part, front, 9 + 4 * turn, self.mate).start()

    def fifth(self, part):
        for turn, a_slot in enumerate((self.c, self.other_high)):
            far = self.along_x(a_slot, 4)
            self.wait_a(part, far)
            self.copy_a(part, far, 10 + 4 * turn, self.mate).start()

    def finish(self, part):
        for b_slot in (self.other_row, self.r):
            self.wait_b(part, self.along_y(b_slot, self.ahead))
            self.wait_b(part, self.along_y(b_slot, 4))
        for a_slot in (self.c, self.other_high):
            for shift in range(0, self.half, 2):
                self.wait_a(part, self.along_x(a_slot + self.turned, shift))
        for number in range(15):
            self.copy_a(part, self.c, number, self.mate).wait_send()
        for number in range(8):
            self.copy_b(part, self.r, number, (self.other_row, self.c)).wait_send()


def column_attention(
    x_ref,
    feat_ref,
    wq_ref,
    wk_ref,
    wv_ref,
    wg_ref,
    wo_ref,
    we_ref,
    ws_ref,
    factor_ref,
    row_ref,
    column_ref,
    out_ref,
    a_out,
    b_out,
    q_scr,
    kt_scr,
    v_scr,
    acc_scr,
    own_scr,
    a_all,
    b_all,
    a_send,
    a_recv,
    b_send,
    b_recv,
    out_sem,
):
    step = pl.program_id(0)
    seqs = x_ref.shape[1]
    spread = Spread(own_scr, a_all, b_all, a_send, a_recv, b_send, b_recv)

    @pl.when(step == 0)
    def _():
        feat = feat_ref[...]
        a_all[spread.c, 0] = jnp.zeros((32, seqs), jnp.bfloat16)
        own_scr[0] = jnp.zeros((32, seqs), jnp.bfloat16)
        a_all[spread.c, 0, :16, :128] = mm(feat, row_ref[...]).astype(jnp.bfloat16)
        own_scr[0, :16, :128] = mm(feat, column_ref[...]).astype(jnp.bfloat16)
        spread.greet()
        spread.begin(0)

    x = x_ref[0].astype(jnp.float32)
    normed = standardize_features(x).astype(jnp.bfloat16)
    q_scr[...] = mm(normed, wq_ref[...]).astype(jnp.bfloat16)
    kt_scr[...] = mm(normed, wk_ref[...]).T.astype(jnp.bfloat16)
    v = mm(normed, wv_ref[...]).astype(jnp.bfloat16)
    ones = jnp.ones((seqs, 128), jnp.bfloat16)
    v_scr[0] = jnp.concatenate([v[:, :128], ones], axis=1)
    v_scr[1] = jnp.concatenate([v[:, 128:], ones], axis=1)
    lane = lax.broadcasted_iota(jnp.int32, (seqs, 256), 1)
    factor = math.log2(math.e) / math.sqrt(HEAD)

    for group in range(2):
        total = None
        for k in range(HEADS // 2):
            q = jnp.where(
                lane // HEAD == group * 4 + k, q_scr[...], jnp.zeros((), jnp.bfloat16)
            )
            scores = mm(q, kt_scr[...])
            top = jnp.max(scores, axis=-1, keepdims=True)
            weights = jnp.exp2((scores - top) * factor).astype(jnp.bfloat16)
            values = jnp.where(
                lane % 128 // HEAD == k, v_scr[group], jnp.zeros((), jnp.bfloat16)
            )
            part = mm(weights, values)
            total = part if total is None else total + part
        acc_scr[group] = total
    attended = jnp.concatenate(
        [
            acc_scr[0, :, :128] / acc_scr[0, :, 128:],
            acc_scr[1, :, :128] / acc_scr[1, :, 128:],
        ],
        axis=1,
    )
    gate = jax.nn.sigmoid(mm(normed, wg_ref[...]))
    mixed = (attended * gate).astype(jnp.bfloat16)
    first = x + mm(mixed, wo_ref[...])
    hidden = jnp.maximum(
        mm(standardize_features(first).astype(jnp.bfloat16), we_ref[...]), 0.0
    ).astype(jnp.bfloat16)
    second = first + mm(hidden, ws_ref[...])
    out_ref[...] = second.astype(jnp.bfloat16)
    factors = mm(standardize_features(second).astype(jnp.bfloat16), factor_ref[...])
    turned = factors.T.astype(jnp.bfloat16)
    a_all[spread.c, step + 1] = turned[:32]
    own_scr[step + 1] = turned[32:64]
    spread.second(step)
    spread.begin(step + 1)

    @pl.when(step > 0)
    def _():
        spread.third(step - 1)

    @pl.when(step > 1)
    def _():
        spread.fourth(step - 2)

    @pl.when(step > 2)
    def _():
        spread.fifth(step - 3)

    last = pl.num_programs(0)

    @pl.when(step == last - 1)
    def _():
        spread.third(last - 1)
        spread.fourth(last - 2)
        spread.fifth(last - 3)
        spread.second(last)
        spread.fourth(last - 1)
        spread.fifth(last - 2)
        spread.third(last)
        spread.fifth(last - 1)
        spread.fourth(last)
        spread.fifth(last)
        for part in range(5):
            spread.finish(part)
        results = [
            pltpu.make_async_copy(a_all, a_out, out_sem.at[0]),
            pltpu.make_async_copy(b_all, b_out, out_sem.at[1]),
        ]
        for copy in results:
            copy.start()
        for copy in results:
            copy.wait()


def run_attention(x, feat, weights, interpret=False):
    count_res, seqs, width = x.shape
    whole = [resident(one.shape) for one in (feat,) + weights]
    return pl.pallas_call(
        column_attention,
        grid=(count_res,),
        in_specs=[pl.BlockSpec((1, seqs, width), lambda i: (i, 0, 0))] + whole,
        out_specs=[
            pl.BlockSpec((seqs, width), lambda i: (0, i)),
            pl.BlockSpec(memory_space=pl.ANY),
            pl.BlockSpec(memory_space=pl.ANY),
        ],
        out_shape=[
            jax.ShapeDtypeStruct((seqs, count_res * width), jnp.bfloat16),
            jax.ShapeDtypeStruct((16, count_res + 1, 32, seqs), jnp.bfloat16),
            jax.ShapeDtypeStruct((8, count_res + 1, 32, seqs), jnp.bfloat16),
        ],
        scratch_shapes=[
            pltpu.VMEM((seqs, width), jnp.bfloat16),
            pltpu.VMEM((width, seqs), jnp.bfloat16),
            pltpu.VMEM((2, seqs, width), jnp.bfloat16),
            pltpu.VMEM((2, seqs, width), jnp.float32),
            pltpu.VMEM((count_res + 1, 32, seqs), jnp.bfloat16),
            pltpu.VMEM((16, count_res + 1, 32, seqs), jnp.bfloat16),
            pltpu.VMEM((8, count_res + 1, 32, seqs), jnp.bfloat16),
            pltpu.SemaphoreType.DMA((count_res + 1, 15)),
            pltpu.SemaphoreType.DMA((count_res + 1, 16)),
            pltpu.SemaphoreType.DMA((count_res + 1, 8)),
            pltpu.SemaphoreType.DMA((count_res + 1, 8)),
            pltpu.SemaphoreType.DMA((2,)),
        ],
        compiler_params=pltpu.CompilerParams(
            dimension_semantics=("arbitrary",),
            vmem_limit_bytes=VMEM_LIMIT,
            collective_id=0,
            has_side_effects=True,
        ),
        name="column_attention",
    )(x, feat, *weights)


def pair_tile(
    a_ref,
    b_ref,
    offset_ref,
    project_ref,
    expand_ref,
    shrink_ref,
    bins_ref,
    pair_ref,
    distogram_ref,
    c_scr,
    x_scr,
    right_scr,
    own_scr,
    out_scr,
    in_scr,
    turn_scr,
    send_sem,
    recv_sem,
):
    step = pl.program_id(0)
    seqs = b_ref.shape[3]
    r, c = lax.axis_index("row"), lax.axis_index("col")
    mirror_row, parity = c // 2, c % 2
    diagonal = mirror_row == r
    barrier = pltpu.get_barrier_semaphore()

    def mirror_copy(number):
        return pltpu.make_async_remote_copy(
            src_ref=out_scr.at[number],
            dst_ref=in_scr.at[parity, number % 2],
            send_sem=send_sem.at[number],
            recv_sem=recv_sem.at[parity, number % 2],
            device_id=(mirror_row, 2 * r + number // 2),
            device_id_type=MESH,
        )

    def stays(number):
        return jnp.logical_and(diagonal, number // 2 == parity)

    def dispatch(number):
        @pl.when(jnp.logical_not(stays(number)))
        def _():
            mirror_copy(number).start()

    @pl.when(step == 0)
    def _():
        for h in range(2):

            @pl.when(jnp.logical_not(jnp.logical_and(diagonal, parity == h)))
            def _(h=h):
                pl.semaphore_signal(
                    barrier, inc=1, device_id=(mirror_row, 2 * r + h), device_id_type=MESH
                )

    @pl.when(step == 1)
    def _():
        pl.semaphore_wait(barrier, 2 - jnp.where(diagonal, 1, 0))

    @pl.when(step == 0)
    def _():
        for d in range(8):
            right_scr[4 * d : 4 * d + 4, :] = b_ref[d, 0, :16, :128].astype(jnp.float32)[:4]

    factors = a_ref[pl.ds(4 * step, 4), 1:].reshape(512, seqs)
    outer = lax.dot_general(
        b_ref[:, 1:].reshape(1024, seqs),
        factors,
        (((1,), (1,)), ((), ())),
        preferred_element_type=jnp.float32,
    )
    for part in range(4):
        c_scr[part] = outer[:, 128 * part : 128 * part + 128]

    @pl.when(step > 0)
    def _():
        dispatch(step - 1)

    for part in range(4):
        block = (c_scr[part].reshape(32, 32, 128) * (1.0 / seqs)).astype(jnp.bfloat16)
        x_scr[128 * part : 128 * part + 128, :] = jnp.concatenate(
            [block[:, :, 32 * i : 32 * i + 32].reshape(32, 1024) for i in range(4)], axis=0
        )
    projected = mm(x_scr[...], project_ref[...])
    index = lax.broadcasted_iota(jnp.int32, (512, 128), 0)
    bins = lax.broadcasted_iota(jnp.int32, (512, 128), 1)
    offset = (c * 32 + index % 32) - (r * 64 + step * 16 + index // 32)
    onehot = jnp.where(jnp.clip(offset, -CLIP, CLIP) + CLIP == bins, 1.0, 0.0)
    relative = mm(onehot.astype(jnp.bfloat16), offset_ref[...])
    left = []
    for n in range(4):
        four = a_ref[4 * step + n, 0, :16, :128].astype(jnp.float32)
        left += [four[i : i + 1] for i in range(4)]
    right = right_scr[...]
    embedded = jnp.concatenate([right + one for one in left], axis=0)
    start = embedded + relative + projected
    hidden = jnp.maximum(
        mm(standardize_features(start).astype(jnp.bfloat16), expand_ref[...]), 0.0
    ).astype(jnp.bfloat16)
    final = (start + mm(hidden, shrink_ref[...])).astype(jnp.bfloat16)
    pair_ref[...] = final.reshape(16, 32, 128)
    logits = mm(final, bins_ref[...])
    own_scr[step] = logits
    packed = jnp.where(bins[:256] < 64, logits[:256], logits[256:]).astype(jnp.bfloat16)
    out_scr[step] = packed

    @pl.when(stays(step))
    def _():
        in_scr[parity, step % 2] = packed

    @pl.when(step == pl.num_programs(0) - 1)
    def _():
        dispatch(step)
        for quarter in range(2):
            for k in range(2):

                @pl.when(jnp.logical_not(jnp.logical_and(diagonal, parity == k)))
                def _(k=k, quarter=quarter):
                    pltpu.make_async_remote_copy(
                        src_ref=in_scr.at[k, quarter],
                        dst_ref=in_scr.at[k, quarter],
                        send_sem=recv_sem.at[k, quarter],
                        recv_sem=recv_sem.at[k, quarter],
                        device_id=(mirror_row, 2 * r + k),
                        device_id_type=MESH,
                    ).wait_recv()

                for i in range(8):
                    rows = in_scr[k, quarter, 32 * i : 32 * i + 32, :].astype(jnp.float32)
                    first = k * 1024 + quarter * 16 + i
                    turn_scr[pl.ds(first, 32, stride=32), :] = rows
                    turn_scr[pl.ds(first + 8, 32, stride=32), :] = pltpu.roll(rows, 64, 1)
        for number in range(4):
            total = own_scr[number] + turn_scr[512 * number : 512 * number + 512, :]
            distogram_ref[16 * number : 16 * number + 16] = (
                total[:, :64].astype(jnp.bfloat16).reshape(16, 32, 64)
            )
        for number in range(4):

            @pl.when(jnp.logical_not(stays(number)))
            def _(number=number):
                mirror_copy(number).wait_send()


def run_pair(a_all, b_all, offset, project, expand, shrink, bins):
    return pl.pallas_call(
        pair_tile,
        grid=(4,),
        in_specs=[FULL, FULL]
        + [resident(one.shape) for one in (offset, project, expand, shrink, bins)],
        out_specs=[
            pl.BlockSpec((16, 32, 128), lambda i: (i, 0, 0)),
            pl.BlockSpec((64, 32, 64), lambda i: (0, 0, 0)),
        ],
        out_shape=[
            jax.ShapeDtypeStruct((64, 32, 128), jnp.bfloat16),
            jax.ShapeDtypeStruct((64, 32, 64), jnp.bfloat16),
        ],
        scratch_shapes=[
            pltpu.VMEM((4, 1024, 128), jnp.float32),
            pltpu.VMEM((512, 1024), jnp.bfloat16),
            pltpu.VMEM((32, 128), jnp.float32),
            pltpu.VMEM((4, 512, 128), jnp.float32),
            pltpu.VMEM((4, 256, 128), jnp.bfloat16),
            pltpu.VMEM((2, 2, 256, 128), jnp.bfloat16),
            pltpu.VMEM((2048, 128), jnp.float32),
            pltpu.SemaphoreType.DMA((4,)),
            pltpu.SemaphoreType.DMA((2, 2)),
        ],
        compiler_params=pltpu.CompilerParams(
            dimension_semantics=("arbitrary",),
            vmem_limit_bytes=VMEM_LIMIT,
            collective_id=1,
            has_side_effects=True,
        ),
        name="pair_tile",
    )(a_all, b_all, offset, project, expand, shrink, bins)


def shards(
    homolog_stack,
    per_amino_features,
    asking_matrix,
    lookup_matrix,
    content_matrix,
    sigmoid_scaling_matrix,
    attention_result_matrix,
    stack_transition_expand_matrix,
    stack_transition_shrink_matrix,
    former_factor_matrix,
    latter_factor_matrix,
    factor_mean_projection,
    row_amino_embedding,
    column_amino_embedding,
    offset_embedding_matrix,
    grid_transition_expand,
    grid_transition_shrink,
    distance_bins_matrix,
):
    rows = lax.axis_size("row")
    cols = lax.axis_size("col")
    whole = rows * cols
    seq_here, residues, width = homolog_stack.shape
    res_here = residues // whole
    fragments = homolog_stack.reshape(1, seq_here, whole, res_here, width)
    moved = lax.all_to_all(fragments, ("row", "col"), split_axis=2, concat_axis=0, tiled=True)
    local = moved.reshape(-1, res_here, width)
    seqs = local.shape[0]
    both = jnp.concatenate(
        [former_factor_matrix, latter_factor_matrix, jnp.zeros((width, 64), jnp.bfloat16)], axis=1
    )
    updated, a_all, b_all = run_attention(
        local.transpose(1, 0, 2),
        jnp.pad(per_amino_features, ((0, 12), (0, 0))),
        (
            asking_matrix,
            lookup_matrix,
            content_matrix,
            sigmoid_scaling_matrix,
            attention_result_matrix,
            stack_transition_expand_matrix,
            stack_transition_shrink_matrix,
            both,
            row_amino_embedding,
            column_amino_embedding,
        ),
    )
    alignment_output = updated.reshape(seqs, res_here, width)
    factor = former_factor_matrix.shape[1]
    project = (
        factor_mean_projection.reshape(factor, factor, -1)
        .transpose(1, 0, 2)
        .reshape(factor * factor, -1)
    )
    pair_output, distogram = run_pair(
        a_all,
        b_all,
        jnp.pad(offset_embedding_matrix, ((0, 127 - 2 * CLIP), (0, 0))),
        project,
        grid_transition_expand,
        grid_transition_shrink,
        jnp.concatenate([distance_bins_matrix] * 2, axis=1),
    )
    return (alignment_output, pair_output, distogram)


def solution(mesh):
    placed = (P(("row", "col"), None, None), P(("row", "col"), None)) + (P(),) * 16
    return jax.shard_map(
        shards,
        mesh=mesh,
        in_specs=placed,
        out_specs=(P(None, ("row", "col"), None), P("row", "col", None), P("row", "col", None)),
        check_vma=False,
    )
```
